32 devices in a mesh: fsdp: 8 (over z, y), tp: 4 (over x, core).
Axes of the slice: x: 2, y: 2, z: 4, core: 2. Of those that a mesh axis runs over, the one named last changes fastest.
Arguments:
- inputs: bfloat16 [2, 4096, 1280], P(None, ('fsdp', 'tp')), may hold values from -6 to 6
- cotangent: bfloat16 [2, 4096, 1280], P(None, ('fsdp', 'tp')), may hold values from -6 to 6
- segment_ids: int32 [2, 4096], P(None, 'fsdp'), may hold values from 0 to 103, as said below
- parents: int32 [2, 104], P(None, 'fsdp'), may hold values from 0 to 103, as said below
- positions: int32 [2, 4096], P(None, 'fsdp'), may hold values from 0 to 191, as said below
- norm1_gain: bfloat16 [1280], P(('fsdp', 'tp')), may hold values from 0.5 to 1.5
- w_query: bfloat16 [1280, 1280], P('fsdp', 'tp'), may hold values from -0.15625 to 0.15625
- w_key: bfloat16 [1280, 320], P(('fsdp', 'tp')), may hold values from -0.15625 to 0.15625
- w_value: bfloat16 [1280, 320], P(('fsdp', 'tp')), may hold values from -0.15625 to 0.15625
- w_out: bfloat16 [1280, 1280], P('tp', 'fsdp'), may hold values from -0.625 to 0.625
- norm2_gain: bfloat16 [1280], P(('fsdp', 'tp')), may hold values from 0.5 to 1.5
- w_gate: bfloat16 [1280, 3584], P('fsdp', 'tp'), may hold values from -0.15625 to 0.15625
- w_up: bfloat16 [1280, 3584], P('fsdp', 'tp'), may hold values from -0.15625 to 0.15625
- w_down: bfloat16 [3584, 1280], P('tp', 'fsdp'), may hold values from -0.09375 to 0.09375
Outputs:
- output: bfloat16 [2, 4096, 1280], P(None, ('fsdp', 'tp'))
- grad_input: float32 [2, 4096, 1280], P(None, ('fsdp', 'tp'))
- grad_norm1: float32 [1280], P(('fsdp', 'tp'))
- grad_query: float32 [1280, 1280], P('fsdp', 'tp')
- grad_key: float32 [1280, 320], P(('fsdp', 'tp'))
- grad_value: float32 [1280, 320], P(('fsdp', 'tp'))
- grad_out: float32 [1280, 1280], P('tp', 'fsdp')
- grad_norm2: float32 [1280], P(('fsdp', 'tp'))
- grad_gate: float32 [1280, 3584], P('fsdp', 'tp')
- grad_up: float32 [1280, 3584], P('fsdp', 'tp')
- grad_down: float32 [3584, 1280], P('tp', 'fsdp')
The draws below stay inside these ranges and needn't reach their ends.
Inputs may be any that keep to these rules, and one draw needn't show every extreme that they name: `segment_ids`: each tree of 512 consecutive tokens holds 13 segments: a trunk of 128 tokens, 4 branches and 8 leaves of 32 tokens each, two leaves on each branch. The segments of tree t are numbered 13 t to 13 t + 12 in an order drawn anew for every tree, the trunk first in the layout and the others in a drawn order. The parent of a trunk is the trunk itself, of a branch its tree's trunk, of a leaf its branch; parents stay in their segment's tree. `positions`: positions count along a token's path: a trunk from 0, a branch from 128, a leaf from 160, rising by one within a segment in token order.
All inputs are finite; a program needn't handle non-finite values.
Results may differ from the reference program's by a relative error of at most 0.018.
Values may be sent and summed in bfloat16 or wider, within the bound.
A program may use at most 128 MiB of HBM per device.

```python
import jax
import jax.numpy as jnp
import numpy as np
from jax import lax

D = 1280
H = 20
KV = 5
HD = 64
FF = 3584
SEG = 32
MB = 2
TRUNK = 128
TREE = 512
TREES = 8
TOKENS = 4096
SEGS = 104


PARENT_OF = np.array([0, 0, 0, 0, 0, 1, 1, 2, 2, 3, 3, 4, 4], dtype=np.int32)


def tree_layout(key):
    tree_count = MB * TREES
    key_list = jax.random.split(jax.random.fold_in(key, 4711), 2 * tree_count)
    labels = jax.vmap(lambda subkey: jax.random.permutation(subkey, 13))(key_list[:tree_count]).astype(jnp.int32)
    orders = jax.vmap(lambda subkey: jax.random.permutation(subkey, 12))(key_list[tree_count:]).astype(jnp.int32)
    offset = jnp.arange(tree_count, dtype=jnp.int32) % TREES * 13
    places = jnp.arange(TREE, dtype=jnp.int32)
    inner_place = jnp.maximum(places - TRUNK, 0)
    slot_index = jnp.minimum(inner_place // SEG, 11)
    structure = jnp.where(places[None, :] < TRUNK, 0, 1 + jnp.take(orders, slot_index, axis=1)).astype(jnp.int32)
    depth_start = jnp.where(structure <= 4, TRUNK, TRUNK + SEG)
    positions = jnp.where(places[None, :] < TRUNK, places[None, :], depth_start + inner_place[None, :] % SEG).astype(jnp.int32)
    segment_ids = offset[:, None] + jnp.take_along_axis(labels, structure, axis=1)
    inverse = jnp.argsort(labels, axis=1).astype(jnp.int32)
    parent_structure = jnp.asarray(PARENT_OF)[inverse]
    parents = offset[:, None] + jnp.take_along_axis(labels, parent_structure, axis=1)
    return (segment_ids.reshape(MB, TOKENS), parents.reshape(MB, SEGS), positions.reshape(MB, TOKENS))


def draw_segment_ids(key, part):
    return tree_layout(key)[0]


def draw_parents(key, part):
    return tree_layout(key)[1]


def draw_positions(key, part):
    return tree_layout(key)[2]


def raised(result, key, source, target, blocks, factor):
    def block_of(dim):
        return (jnp.arange(result.shape[dim]) // (result.shape[dim] // blocks)).reshape((-1,) + (1,) * (result.ndim - 1 - dim))

    near = jax.random.permutation(key, blocks)[block_of(target)]
    second = (block_of(target) + blocks // 2) % blocks
    return jnp.where((block_of(source) == near) | (block_of(source) == second), factor * result, result)


def level_of(key, extent, cuts, smallest, largest):
    factor_of = 1.0
    for axis_at, shards_of in cuts:
        steps = jax.random.uniform(jax.random.fold_in(jax.random.fold_in(key, 6), axis_at), (shards_of,), jnp.float32, smallest / len(cuts), largest / len(cuts))
        factor_of = factor_of * jnp.repeat(jnp.exp(steps), extent[axis_at] // shards_of).reshape((-1,) + (1,) * (len(extent) - 1 - axis_at))
    return factor_of


def noise(key, dims, width, limit, cuts=(), kind=jnp.bfloat16):
    factor_of = level_of(key, dims, cuts, -0.22, 0.18) if cuts else 1.0
    values = jax.random.normal(key, dims, jnp.float32) * width * factor_of
    return jnp.minimum(jnp.maximum(values, -limit), limit).astype(kind)


def bell_draw_with(own_key, shape, width, most, cuts, heavy, kind=jnp.bfloat16):
    drawn = width * jax.random.normal(own_key, shape, jnp.float32)
    if cuts:
        drawn = drawn * level_of(own_key, shape, cuts, -0.22, 0.18)
    return jnp.clip(raised(drawn, jax.random.fold_in(own_key, 3), *heavy), -most, most).astype(kind)


def setup_inputs(seed: int = 0) -> dict:
    key_of = jax.random.split(jax.random.key(seed), 15)
    return {
        "inputs": noise(key_of[0], (MB, TOKENS, D), 1.0, 6.0, ((1, 32),)),
        "cotangent": bell_draw_with(key_of[1], (MB, TOKENS, D), 1.0, 6.0, ((1, 32),), (1, 2, 32, 2.75)),
        "segment_ids": draw_segment_ids(jax.random.fold_in(key_of[14], 71), 0),
        "parents": draw_parents(jax.random.fold_in(key_of[14], 71), 0),
        "positions": draw_positions(jax.random.fold_in(key_of[14], 71), 0),
        "norm1_gain": jnp.clip(1.0 + 0.1 * jax.random.normal(key_of[5], (D,), jnp.float32), 0.5, 1.5).astype(jnp.bfloat16),
        "w_query": noise(key_of[6], (D, H * HD), D ** -0.5, 0.15625, ((0, 8), (1, 4))),
        "w_key": noise(key_of[7], (D, KV * HD), D ** -0.5, 0.15625, ((0, 32),)),
        "w_value": noise(key_of[8], (D, KV * HD), D ** -0.5, 0.15625, ((0, 32),)),
        "w_out": noise(key_of[9], (H * HD, D), (H * HD // 16) ** -0.5, 0.625, ((0, 4), (1, 8))),
        "norm2_gain": jnp.clip(1.0 + 0.1 * jax.random.normal(key_of[10], (D,), jnp.float32), 0.5, 1.5).astype(jnp.bfloat16),
        "w_gate": noise(key_of[11], (D, FF), D ** -0.5, 0.15625, ((0, 8), (1, 4))),
        "w_up": noise(key_of[12], (D, FF), D ** -0.5, 0.15625, ((0, 8), (1, 4))),
        "w_down": noise(key_of[13], (FF, D), FF ** -0.5, 0.09375, ((0, 4), (1, 8))),
    }


@jax.custom_vjp
def low(v):
    return lax.optimization_barrier(v.astype(jnp.bfloat16)).astype(jnp.float32)

@jax.custom_vjp
def low_back(v):
    return v

def low_keep(v):
    return (low(v), None)

def low_pass(kept, grad):
    return (grad,)

def back_keep(v):
    return (v, None)

def back_low(kept, grad):
    return (low(grad),)
low.defvjp(low_keep, low_pass)
low_back.defvjp(back_keep, back_low)
EPSILON = 1e-05
ROPE_BASE = 10000.0
MASKED = -1e+30
HIGHEST = lax.Precision.HIGHEST

def norm_scale(values):
    return lax.rsqrt(lax.optimization_barrier(jnp.mean(values * values, axis=-1, keepdims=True)) + EPSILON)

def rotate(values, places):
    half_width = HD // 2
    frequency = 1.0 / ROPE_BASE ** (jnp.arange(half_width, dtype=jnp.float32) / half_width)
    angles = places.astype(jnp.float32)[..., None] * frequency
    cosine = jnp.cos(angles)[..., None, :]
    sine_part = jnp.sin(angles)[..., None, :]
    shaped = values.reshape(values.shape[:-1] + (values.shape[-1] // HD, HD))
    first_half = shaped[..., :half_width]
    second_half = shaped[..., half_width:]
    turned = jnp.concatenate([first_half * cosine - second_half * sine_part, second_half * cosine + first_half * sine_part], axis=-1)
    return turned.reshape(values.shape)

def tree_attention(pieces):
    queries, keys_all, values_all, segment, places, table = pieces
    group_size = H // KV
    query_heads = queries.reshape(TREE, KV, group_size, HD)
    key_heads = keys_all.reshape(TREE, KV, HD)
    value_heads = values_all.reshape(TREE, KV, HD)
    raw_scores = jnp.einsum('qgjd,kgd->gjqk', query_heads, key_heads, precision=HIGHEST)
    scores = low_back(raw_scores) * HD ** (-0.5)
    parent = jnp.take(table, segment)
    grand_parent = jnp.take(table, parent)
    allowed = ((segment[None, :] == segment[:, None]) | (segment[None, :] == parent[:, None]) | (segment[None, :] == grand_parent[:, None])) & (places[None, :] <= places[:, None])
    scores = jnp.where(allowed, scores, MASKED)
    row_peak = lax.optimization_barrier(jnp.max(scores, axis=-1, keepdims=True))
    weights_row = jnp.exp(scores - row_peak)
    probability = weights_row / lax.optimization_barrier(jnp.sum(weights_row, axis=-1, keepdims=True))
    mixed = jnp.einsum('gjqk,kgd->qgjd', low(probability), value_heads, precision=HIGHEST)
    return mixed.reshape(TREE, H * HD)

def layer(inputs, gain_one, w_query, w_key, w_value, w_out, gain_two, w_gate, w_up, w_down, segment_ids, parents, positions):
    normed = low(inputs * norm_scale(inputs) * gain_one)
    queries = low(rotate(low_back(jnp.dot(normed, w_query, precision=HIGHEST)), positions))
    keys_all = low(rotate(low_back(jnp.dot(normed, w_key, precision=HIGHEST)), positions))
    values_all = low(low_back(jnp.dot(normed, w_value, precision=HIGHEST)))
    tree_count = MB * TREES
    tables = jnp.repeat(parents, TREES, axis=0)
    blocks = (queries.reshape(tree_count, TREE, H * HD), keys_all.reshape(tree_count, TREE, KV * HD), values_all.reshape(tree_count, TREE, KV * HD), segment_ids.reshape(tree_count, TREE), positions.reshape(tree_count, TREE), tables)
    mixed = lax.map(jax.checkpoint(tree_attention), blocks)
    attended = low(low_back(mixed.reshape(MB, TOKENS, H * HD)))
    hidden = inputs + low_back(jnp.dot(attended, w_out, precision=HIGHEST))
    normed_two = low(hidden * norm_scale(hidden) * gain_two)
    gate_pre = low_back(jnp.dot(normed_two, w_gate, precision=HIGHEST))
    upward = low_back(jnp.dot(normed_two, w_up, precision=HIGHEST))
    product = low(jax.nn.silu(gate_pre) * upward)
    return hidden + low_back(jnp.dot(product, w_down, precision=HIGHEST))

def reference(inputs, cotangent, segment_ids, parents, positions, norm1_gain, w_query, w_key, w_value, w_out, norm2_gain, w_gate, w_up, w_down):
    floats = [value.astype(jnp.float32) for value in (inputs, norm1_gain, w_query, w_key, w_value, w_out, norm2_gain, w_gate, w_up, w_down)]

    def forward(*values):
        return layer(*values, segment_ids, parents, positions)
    output, pullback = jax.vjp(forward, *floats)
    gradients = pullback(cotangent.astype(jnp.float32))
    return (output.astype(jnp.bfloat16), gradients[0], gradients[1], gradients[2], gradients[3], gradients[4], gradients[5], gradients[6], gradients[7], gradients[8], gradients[9])
```

```python
import functools

import jax
import jax.numpy as jnp
from jax import lax
from jax.experimental import pallas as pl
from jax.experimental.pallas import tpu as pltpu
from jax.sharding import PartitionSpec as P

EPSILON = 1e-05
ROPE_BASE = 10000.0
MASKED = -1e30
H = 20
KV = 5
HD = 64
MB = 2
MESH = pl.DeviceIdType.MESH
BF = jnp.bfloat16
F32 = jnp.float32
QKV = 640
AW = 1024


def dot(left, right, left_dim, right_dim):
    return lax.dot_general(
        left, right, (((left_dim,), (right_dim,)), ((), ())), preferred_element_type=F32
    )


def loop(count, body):
    def step(index, carry):
        body(index)
        return carry

    lax.fori_loop(0, count, step, 0)


def rows(index, size, extent):
    return pl.ds(pl.multiple_of(index * size, size), extent)


def swap_halves(values):
    lane = lax.broadcasted_iota(jnp.int32, values.shape, 1)
    return jnp.where(lane % 64 < 32, pltpu.roll(values, 96, 1), pltpu.roll(values, 32, 1))


class Exchange:
    def __init__(self, k, tag, whole, base, source=None):
        own, near, far = k.t, k.x * 2 + 1 - k.c, (1 - k.x) * 2 + k.c
        self.whole = whole

        def block(rank):
            return whole.at[pl.ds(pl.multiple_of(base + rank * 128, 128), 128)]

        src = block(own) if source is None else source
        self.to_sib = pltpu.make_async_remote_copy(
            src, block(own), k.ex_s.at[tag, 0], k.ex_r.at[tag, 0], (k.f, k.sib), MESH)
        self.to_far = pltpu.make_async_remote_copy(
            src, block(own), k.ex_s.at[tag, 1], k.ex_r.at[tag, 1], (k.f, k.far), MESH)
        self.relay = pltpu.make_async_remote_copy(
            block(far), block(far), k.ex_s.at[tag, 2], k.ex_r.at[tag, 2], (k.f, k.sib), MESH)

    def start(self):
        self.to_far.start()
        self.to_sib.start()

    def forward(self):
        self.to_far.wait_recv()
        self.relay.start()

    def finish(self):
        self.to_sib.wait_recv()
        self.relay.wait_recv()

    def drain(self):
        self.to_far.wait_send()
        self.to_sib.wait_send()
        self.relay.wait_send()


class TreeSum:
    def __init__(self, k, tag, keep, b):
        self.k, self.b, self.keep = k, b, keep
        self.inner = pltpu.make_async_remote_copy(
            k.part.at[b, 1 - k.c], k.near.at[keep, b], k.ts_s.at[tag, 0], k.ts_r.at[tag, 0], (k.f, k.sib), MESH)
        self.outer = pltpu.make_async_remote_copy(
            k.half.at[keep, b], k.far_in.at[keep, b], k.ts_s.at[tag, 1], k.ts_r.at[tag, 1], (k.f, k.far), MESH)

    def start(self):
        self.inner.start()

    def middle(self):
        k, b, keep = self.k, self.b, self.keep
        self.inner.wait_recv()
        other = 1 - k.x

        def body(i):
            r = rows(i, 32, 32)
            k.half[keep, b, r, :] = (
                k.part[b, k.c, other, r, :].astype(F32) + k.near[keep, b, other, r, :].astype(F32)
            ).astype(BF)

        loop(4, body)
        self.outer.start()

    def wait(self):
        self.outer.wait_recv()

    def value(self, r):
        k, b, keep = self.k, self.b, self.keep
        return (
            k.part[b, k.c, k.x, r, :].astype(F32)
            + k.near[keep, b, k.x, r, :].astype(F32)
            + k.far_in[keep, b, r, :].astype(F32)
        )

    def drain(self):
        self.inner.wait_send()
        self.outer.wait_send()


class RingGather:
    def __init__(self, k, tag, whole, lane, width):
        self.k, self.tag, self.whole, self.lane, self.width = k, tag, whole, lane, width
        self.step = 0

    def copy(self, way, s):
        k = self.k
        spot = k.at_ring((k.p + (k.n - s if way == 0 else s)) % k.n)
        half = k.shard // 2
        where = pl.ds(pl.multiple_of(spot * k.shard + way * half, 16), half)
        ref = self.whole.at[where, pl.ds(self.lane, self.width)]
        return pltpu.make_async_remote_copy(
            ref, ref, k.ga_s.at[self.tag * 2 + way, s], k.ga_r.at[self.tag * 2 + way, s],
            (k.next if way == 0 else k.prev, k.t), MESH)

    def start(self):
        for way in (0, 1):
            self.copy(way, 0).start()

    def pump(self):
        s = self.step
        self.step += 1
        for way in (0, 1):
            self.copy(way, s).wait_recv()
            if s < self.k.n - 2:
                self.copy(way, s + 1).start()

    def drain(self):
        if self.step:
            self.step = 0
            for s in range(self.k.n - 1):
                for way in (0, 1):
                    self.copy(way, s).wait_send()


class RingSum:
    def __init__(self, k, tag, grad, lane, width, slots, result, out_lane):
        self.k, self.tag, self.grad, self.lane, self.width = k, tag, grad, lane, width
        self.slots, self.result, self.out_lane = slots, result, out_lane
        self.step = 0

    def own(self, way, s):
        k = self.k
        spot = k.at_ring((k.p + (2 * k.n - 1 - s if way == 0 else 1 + s)) % k.n)
        half = k.shard // 2
        return pl.ds(pl.multiple_of(spot * k.shard + way * half, 16), half)

    def copy(self, way, s):
        k = self.k
        if s == 0:
            src = self.grad.at[self.own(way, 0), pl.ds(self.lane, self.width)]
        else:
            src = self.slots.at[way, s - 1, :, pl.ds(self.lane, self.width)]
        return pltpu.make_async_remote_copy(
            src, self.slots.at[way, s, :, pl.ds(self.lane, self.width)],
            k.rs_s.at[self.tag * 2 + way, s], k.rs_r.at[self.tag * 2 + way, s],
            (k.next if way == 0 else k.prev, k.t), MESH)

    def start(self):
        for way in (0, 1):
            self.copy(way, 0).start()

    def pump(self):
        k, s = self.k, self.step
        self.step += 1
        lanes = pl.ds(self.lane, self.width)
        for way in (0, 1):
            self.copy(way, s).wait_recv()
            total = self.slots[way, s, :, lanes].astype(F32) + self.grad[self.own(way, s + 1), lanes].astype(F32)
            if s < k.n - 2:
                self.slots[way, s, :, lanes] = total.astype(BF)
                self.copy(way, s + 1).start()
            else:
                half = k.shard // 2
                self.result[way * half:(way + 1) * half, self.out_lane:self.out_lane + self.width] = total

    def drain(self):
        for s in range(self.k.n - 1):
            for way in (0, 1):
                self.copy(way, s).wait_send()


class Kernel:
    pass


def layer_kernel(n, shard, names, debug, stop, *refs):
    k = Kernel()
    for name, ref in zip(names, refs):
        setattr(k, name, ref)
    k.n, k.shard = n, shard
    f, t = lax.axis_index("fsdp"), lax.axis_index("tp")
    k.f, k.t, k.x, k.c = f, t, t // 2, t % 2
    k.sib = k.x * 2 + 1 - k.c
    k.far = (1 - k.x) * 2 + k.c
    cross = (1 - k.x) * 2 + 1 - k.c
    even = 1 - f % 2
    k.p = even * (f // 2) + (1 - even) * (n - 1 - f // 2)

    def at_ring(place):
        high = place // (n // 2)
        return (1 - high) * (2 * place) + high * (2 * (n - 1 - place) + 1)

    k.at_ring = at_ring
    k.next, k.prev = at_ring((k.p + 1) % n), at_ring((k.p + n - 1) % n)

    barrier = pltpu.get_barrier_semaphore()
    for peer in ((f, k.sib), (f, k.far), (f, cross), (k.next, t), (k.prev, t)):
        pl.semaphore_signal(barrier, inc=1, device_id=peer, device_id_type=MESH)

    mine = pl.ds(pl.multiple_of(f * shard, 16), shard)
    locals_ = [
        pltpu.make_async_copy(k.gate, k.wgu.at[mine, pl.ds(0, 896)], k.loc.at[0]),
        pltpu.make_async_copy(k.up, k.wgu.at[mine, pl.ds(896, 896)], k.loc.at[1]),
        pltpu.make_async_copy(k.down, k.wd.at[mine], k.loc.at[2]),
    ]
    token_copies = []
    for b in range(MB):
        own = pl.ds(pl.multiple_of(b * 512 + t * 128, 128), 128)
        token_copies.append(pltpu.make_async_copy(k.xin.at[b], k.xall.at[own], k.loc.at[3 + b]))
        token_copies.append(pltpu.make_async_copy(k.dyin.at[b], k.dyall.at[own], k.loc.at[5 + b]))
    for copy in locals_ + token_copies:
        copy.start()
    pl.semaphore_wait(barrier, 5)

    kv_copies = []
    for i, peer in enumerate((k.sib, k.far, cross)):
        kv_copies.append(pltpu.make_async_remote_copy(
            k.kv4.at[peer], k.kvr.at[t], k.kv_s.at[i], k.kv_r.at[i], (f, peer), MESH))
    own_kv = pltpu.make_async_copy(k.kv4.at[t], k.kvr.at[t], k.loc.at[7])
    own_kv.start()
    for copy in kv_copies:
        copy.start()
    ex = {}
    for b in range(MB):
        ex["x", b] = Exchange(k, b, k.xall, b * 512, k.xin.at[b])
        ex["dy", b] = Exchange(k, 2 + b, k.dyall, b * 512, k.dyin.at[b])
        ex["n2", b] = Exchange(k, 4 + b, k.n2all, b * 512)
        ex["dh", b] = Exchange(k, 6 + b, k.dyall, b * 512)
    for b in range(MB):
        ex["x", b].start()
    for copy in kv_copies:
        copy.wait_recv()
    own_kv.wait()

    part_rows = shard // 4
    for rank in range(4):
        there = pl.ds(pl.multiple_of(f * shard + rank * part_rows, 8), part_rows)
        here = slice(rank * part_rows, (rank + 1) * part_rows)
        k.stage[here, 0:256] = k.kvr[rank, :, 0:256]
        k.stage[here, 256:512] = k.apre[here, 256:512]
        k.stage[here, 512:640] = k.apre[here, 512:640] + k.kvr[rank, :, 256:384]
        k.stage[here, 640:1024] = k.apre[here, 640:1024]
    to_wa = pltpu.make_async_copy(k.stage, k.wa.at[mine], k.loc.at[8])
    to_wa.start()
    to_wa.wait()
    ring = {
        "kvq": RingGather(k, 0, k.wa, 0, 640),
        "o": RingGather(k, 1, k.wa, 640, 384),
        "g": RingGather(k, 2, k.wgu, 0, 896),
        "u": RingGather(k, 3, k.wgu, 896, 896),
        "d": RingGather(k, 4, k.wd, 0, 896),
    }
    ring["kvq"].start()
    ring["o"].start()
    for copy in locals_:
        copy.wait()

    lane = lax.broadcasted_iota(jnp.int32, (8, 128), 1)[0:1]
    for b in range(MB):
        stacked = jnp.concatenate(
            [k.seg[b:b + 1].astype(F32), k.pos[b:b + 1].astype(F32), jnp.zeros((126, 512), F32)], axis=0)
        columns = stacked.T
        seg_col, pos_col = columns[:, 0:1], columns[:, 1:2]
        first = (f * 13).astype(F32)
        parent = jnp.zeros((512, 1), F32)
        for label in range(13):
            parent = jnp.where(seg_col == first + label, k.par[b, label].astype(F32), parent)
        grand = jnp.zeros((512, 1), F32)
        for label in range(13):
            grand = jnp.where(parent == first + label, k.par[b, label].astype(F32), grand)
        seg_row, pos_row = stacked[0:1], stacked[1:2]
        for i in range(4):
            r = slice(i * 128, (i + 1) * 128)
            same = (
                (seg_row == seg_col[r]) | (seg_row == parent[r]) | (seg_row == grand[r])
            ) & (pos_row <= pos_col[r])
            k.bias[b * 512 + i * 128:b * 512 + (i + 1) * 128, :] = jnp.where(same, 0.0, MASKED).astype(BF)
            angle = pos_col[r] * k.freq[0:1, :]
            sign = jnp.where(lane % 64 < 32, -1.0, 1.0)
            k.cs[b * 512 + i * 128:b * 512 + (i + 1) * 128, 0:128] = jnp.cos(angle)
            k.cs[b * 512 + i * 128:b * 512 + (i + 1) * 128, 128:256] = jnp.sin(angle) * sign

    def first_ring():
        ring["kvq"].pump()
        ring["o"].pump()

    def second_ring():
        ring["g"].pump()
        ring["u"].pump()

    first_ring()
    first_ring()
    for b in range(MB):
        ex["x", b].forward()
    for b in range(MB):
        ex["dy", b].start()
    first_ring()
    ring["g"].start()
    ring["u"].start()
    first_ring()
    first_ring()
    first_ring()
    first_ring()
    for copy in token_copies:
        copy.wait()
    for b in range(MB):
        ex["x", b].finish()

    for i in range(10):
        turned = k.wa[i * 128:(i + 1) * 128, 512:640].astype(F32).T
        k.gains[:, i * 128:(i + 1) * 128] = turned[64:72]

    def normed(r):
        source = k.xall[r, :].astype(F32)
        scale = lax.rsqrt(jnp.mean(source * source, axis=-1, keepdims=True) + EPSILON)
        return source * scale

    def project(b):
        def norm(i):
            k.n2all[rows(i, 64, 64), :] = (normed(pl.ds(pl.multiple_of(b * 512 + i * 64, 64), 64)) * k.gains[0:1, :]).astype(BF)

        loop(8, norm)

        def body(i):
            r = pl.ds(pl.multiple_of(b * 512 + i * 256, 256), 256)
            out = dot(k.n2all[rows(i, 256, 256), :], k.wa[:, 0:QKV], 1, 0)
            cos, sin = k.cs[r, 0:128], k.cs[r, 128:256]
            key = out[:, 0:128]
            key = key * cos + swap_halves(key) * sin
            value = out[:, 128:256]
            k.qkv[r, 0:128] = key.astype(BF)
            k.kvrot[r, 0:128] = pltpu.roll(key, 64, 1).astype(BF)
            k.qkv[r, 128:256] = value.astype(BF)
            k.kvrot[r, 128:256] = pltpu.roll(value, 64, 1).astype(BF)
            for chunk in range(3):
                u = out[:, 256 + chunk * 128:384 + chunk * 128]
                u = (u * cos + swap_halves(u) * sin) * HD ** (-0.5)
                if chunk == 2:
                    u = jnp.where(lax.broadcasted_iota(jnp.int32, u.shape, 1) < 64, u, 0.0)
                k.qkv[r, 256 + chunk * 128:384 + chunk * 128] = u.astype(BF)

        loop(2, body)

    def head_masks(h):
        parity = h % 2
        group = jnp.where(h < 4 - t, 0, 1)
        in_half = (lane // 64 == parity).astype(F32)
        straight = (group == parity).astype(F32)
        return parity, group, in_half, straight

    def pick(b, h, lanes):
        parity, group, in_half, straight = head_masks(h)
        r = slice(b * 512, (b + 1) * 512)
        keep = (in_half * straight).astype(BF)
        turn = (in_half * (1.0 - straight)).astype(BF)
        return k.qkv[r, lanes] * keep + k.kvrot[r, lanes] * turn

    def chunk_of(h, base):
        return pl.ds(pl.multiple_of(base + (h // 2) * 128, 128), 128)

    def attend(b):
        base = b * 512

        def head(h):
            keys, values = pick(b, h, slice(0, 128)), pick(b, h, slice(128, 256))
            q = k.qkv[base:base + 512, chunk_of(h, 256)]
            for low, high, width in ((0, 128, 128), (128, 512, 512)):
                s = dot(q[low:high], keys[0:width], 1, 1) + k.bias[base + low:base + high, 0:width].astype(F32)
                e = jnp.exp(s - jnp.max(s, axis=-1, keepdims=True))
                prob = (e / jnp.sum(e, axis=-1, keepdims=True)).astype(BF)
                k.prob[b * 5 + h, low:high, 0:width] = prob
                out = dot(prob, values[0:width], 1, 0)
                old = k.att[base + low:base + high, chunk_of(h, 0)].astype(F32)
                k.att[base + low:base + high, chunk_of(h, 0)] = (jnp.where(h % 2 == 1, old, 0.0) + out).astype(BF)

        loop(5, head)

    def put_part(b, i, value):
        for c in range(2):
            k.part[b, c, i] = value[c * 128:(c + 1) * 128].astype(BF)

    def two_blocks(b, body):
        def step(i):
            r = pl.ds(pl.multiple_of(b * 512 + i * 256, 256), 256)
            put_part(b, i, body(r))

        loop(2, step)

    sums = {}

    def tree_sum(name, tag, keep, b):
        sums[name, b] = TreeSum(k, tag + b, keep, b)
        sums[name, b].start()

    def out_proj(b):
        two_blocks(b, lambda r: dot(k.att[r, :], k.wa[:, QKV:AW], 1, 1))
        tree_sum("hid", 0, 0, b)

    def finish_hidden(b):
        sums["hid", b].wait()

        def body(i):
            r = rows(i, 32, 32)
            own = pl.ds(pl.multiple_of(b * 512 + t * 128 + i * 32, 32), 32)
            hid = k.xall[own, :].astype(F32) + sums["hid", b].value(r)
            k.hid[pl.ds(pl.multiple_of(b * 128 + i * 32, 32), 32), :] = hid
            scale = lax.rsqrt(jnp.mean(hid * hid, axis=-1, keepdims=True) + EPSILON)
            k.n2all[own, :] = (hid * scale * k.gains[1:2, :]).astype(BF)

        loop(4, body)
        ex["n2", b].start()
        sums["hid", b].drain()

    project(0)
    project(1)
    second_ring()
    attend(0)
    out_proj(0)
    ring["d"].start()
    second_ring()
    attend(1)
    sums["hid", 0].middle()
    out_proj(1)
    second_ring()
    finish_hidden(0)
    sums["hid", 1].middle()
    for b in range(MB):
        ex["dy", b].forward()
    second_ring()
    ex["n2", 0].forward()
    finish_hidden(1)
    second_ring()
    ex["n2", 1].forward()
    for b in range(MB):
        ex["dy", b].finish()
    second_ring()
    second_ring()
    ex["n2", 0].finish()
    if stop != "fwd":
        backward(k, ex, ring, sums, tree_sum, two_blocks, normed, pick, head_masks, chunk_of, cross, kv_copies)
    else:
        ex["n2", 1].finish()
        for _ in range(7):
            ring["d"].pump()
        for name in ("x", "dy", "n2"):
            for b in range(MB):
                ex[name, b].drain()
        for copy in kv_copies:
            copy.wait_send()
    for piece in ring.values():
        piece.drain()
    for i, name in enumerate(debug):
        copy = pltpu.make_async_copy(getattr(k, name), getattr(k, "dbg_" + name), k.loc.at[0])
        copy.start()
        copy.wait()


def backward(k, ex, ring, sums, tree_sum, two_blocks, normed, pick, head_masks, chunk_of, cross, kv_copies):
    f, t, n, shard = k.f, k.t, k.n, k.shard
    lane = lax.broadcasted_iota(jnp.int32, (8, 128), 1)[0:1]
    everything = slice(0, 1024)
    scatter = {
        "d0": RingSum(k, 0, k.gd, 0, 512, k.slot_d, k.out_d, 0),
        "d1": RingSum(k, 1, k.gd, 512, 384, k.slot_d, k.out_d, 512),
        "g0": RingSum(k, 2, k.ggu, 0, 512, k.slot_gu, k.out_g, 0),
        "g1": RingSum(k, 3, k.ggu, 512, 384, k.slot_gu, k.out_g, 512),
        "u0": RingSum(k, 4, k.ggu, 896, 512, k.slot_gu, k.out_u, 0),
        "u1": RingSum(k, 5, k.ggu, 1408, 384, k.slot_gu, k.out_u, 512),
        "o": RingSum(k, 6, k.wgu, 640, 384, k.slot_a, k.out_a, 640),
        "a0": RingSum(k, 7, k.wgu, 0, 512, k.slot_a, k.out_a, 0),
        "a1": RingSum(k, 8, k.wgu, 512, 128, k.slot_a, k.out_a, 512),
    }

    def start(*names):
        for name in names:
            scatter[name].start()

    def pump(*names):
        for name in names:
            scatter[name].pump()

    def gate_up(b):
        def body(i):
            r = pl.ds(pl.multiple_of(b * 512 + i * 128, 128), 128)
            source = k.n2all[r, :]
            gate = dot(source, k.wgu[:, 0:896], 1, 0)
            up = dot(source, k.wgu[:, 896:1792], 1, 0)
            s = 1.0 / (1.0 + jnp.exp(-gate))
            silu = gate * s
            k.m[r, :] = (silu * up).astype(BF)
            k.ab[r, 0:896] = (up * s * (1.0 + gate * (1.0 - s))).astype(BF)
            k.ab[r, 896:1792] = silu.astype(BF)

        loop(4, body)

    def grad_down():
        def body(i):
            k.gd[rows(i, 256, 256), :] = dot(k.dyall[:, rows(i, 256, 256)], k.m[...], 0, 0).astype(BF)

        loop(5, body)

    def hidden_grads(b):
        def body(i):
            r = pl.ds(pl.multiple_of(b * 512 + i * 128, 128), 128)
            product = dot(k.dyall[r, :], k.wd[...], 1, 0)
            k.ab[r, 0:896] = (product * k.ab[r, 0:896].astype(F32)).astype(BF)
            k.ab[r, 896:1792] = (product * k.ab[r, 896:1792].astype(F32)).astype(BF)

        loop(4, body)

    def second_norm_part(b):
        two_blocks(b, lambda r: dot(k.ab[r, :], k.wgu[...], 1, 1))
        tree_sum("dn2", 2, 0, b)

    def grad_gate_up():
        def body(i):
            left = k.n2all[:, rows(i, 256, 256)]
            for low in (0, 896):
                k.ggu[rows(i, 256, 256), low:low + 896] = dot(left, k.ab[:, low:low + 896], 0, 0).astype(BF)

        loop(5, body)

    def finish_hidden_grad(b):
        total = sums["dn2", b]
        total.wait()

        def body(i):
            r = rows(i, 32, 32)
            own = pl.ds(pl.multiple_of(b * 512 + t * 128 + i * 32, 32), 32)
            local = pl.ds(pl.multiple_of(b * 128 + i * 32, 32), 32)
            grad, hid = total.value(r), k.hid[local, :]
            scale = lax.rsqrt(jnp.mean(hid * hid, axis=-1, keepdims=True) + EPSILON)
            k.ggain[1:2, :] += jnp.sum(hid * scale * grad, axis=0, keepdims=True)
            weighted = k.gains[1:2, :] * grad
            dh = (
                k.dyall[own, :].astype(F32)
                + scale * weighted
                - hid * (scale * scale * scale) * jnp.mean(hid * weighted, axis=-1, keepdims=True)
            )
            k.out_x[local, :] = dh
            k.dyall[own, :] = dh.astype(BF)

        loop(4, body)
        ex["dh", b].start()
        total.drain()

    def output_part(b):
        two_blocks(b, lambda r: dot(k.m[r, :], k.wd[...], 1, 1))
        tree_sum("out", 4, 1, b)

    def finish_output(b):
        total = sums["out", b]
        total.wait()

        def body(i):
            r = rows(i, 32, 32)
            local = pl.ds(pl.multiple_of(b * 128 + i * 32, 32), 32)
            k.out_y[local, :] = (k.hid[local, :] + total.value(r)).astype(BF)

        loop(4, body)
        total.drain()

    def grad_out():
        def body(i):
            k.wgu[rows(i, 256, 256), 640:1024] = dot(k.dyall[:, rows(i, 256, 256)], k.att[...], 0, 0).astype(BF)

        loop(5, body)

    def mixed_grad():
        def body(i):
            k.att[rows(i, 256, 256), :] = dot(k.dyall[rows(i, 256, 256), :], k.wa[:, 640:1024], 1, 0).astype(BF)

        loop(4, body)

    def attend_back(b):
        base = b * 512
        k.dq[...] = jnp.zeros_like(k.dq)
        k.dkv[...] = jnp.zeros_like(k.dkv)

        def head(h):
            parity, group, in_half, straight = head_masks(h)
            keys, values = pick(b, h, slice(0, 128)), pick(b, h, slice(128, 256))
            for low, high, width in ((0, 128, 128), (128, 512, 512)):
                q = k.qkv[base + low:base + high, chunk_of(h, 256)]
                grad = k.att[base + low:base + high, chunk_of(h, 0)]
                prob = k.prob[b * 5 + h, low:high, 0:width]
                grad_prob = dot(grad, values[0:width], 1, 1)
                wide = prob.astype(F32)
                delta = jnp.sum(wide * grad_prob, axis=-1, keepdims=True)
                ds = (wide * (grad_prob - delta)).astype(BF)
                k.dq[low:high, chunk_of(h, 0)] += dot(ds, keys[0:width], 1, 0)
                dk = dot(ds, q, 0, 0) * in_half
                dv = dot(prob, grad, 0, 0) * in_half
                k.dkv[0:width, 0:128] += jnp.where(group == parity, dk, pltpu.roll(dk, 64, 1))
                k.dkv[0:width, 128:256] += jnp.where(group == parity, dv, pltpu.roll(dv, 64, 1))

        loop(5, head)

        def body(i):
            r = pl.ds(pl.multiple_of(base + i * 128, 128), 128)
            local = rows(i, 128, 128)
            cos, sin = k.cs[r, 0:128], k.cs[r, 128:256]
            u = k.dkv[local, 0:128]
            k.qkv[r, 0:128] = (u * cos - swap_halves(u) * sin).astype(BF)
            k.qkv[r, 128:256] = k.dkv[local, 128:256].astype(BF)
            for chunk in range(3):
                u = k.dq[local, chunk * 128:(chunk + 1) * 128]
                u = (u * cos - swap_halves(u) * sin) * HD ** (-0.5)
                k.qkv[r, 256 + chunk * 128:384 + chunk * 128] = u.astype(BF)

        loop(4, body)

    def first_norm_part(b):
        two_blocks(b, lambda r: dot(k.qkv[r, :], k.wa[:, 0:QKV], 1, 1))
        tree_sum("dn1", 6, 0, b)

    def first_norm_again(b):
        def body(i):
            r = pl.ds(pl.multiple_of(b * 512 + i * 32, 32), 32)
            unit = normed(r)
            k.dyall[r, :] = (unit * k.gains[0:1, :]).astype(BF)
            spot = pl.ds(pl.multiple_of((i % 4) * 32, 32), 32)
            grad = k.part[b, (i // 4) % 2, i // 8, spot, :].astype(F32)
            k.ggain[0:1, :] += jnp.sum(unit * grad, axis=0, keepdims=True)

        loop(16, body)

    def grad_first():
        def body(i):
            k.wgu[rows(i, 256, 256), 0:QKV] = dot(k.dyall[:, rows(i, 256, 256)], k.qkv[...], 0, 0).astype(BF)

        loop(5, body)
        for i in range(10):
            r = slice(i * 128, (i + 1) * 128)
            turned = jnp.concatenate(
                [jnp.zeros((64, 128), F32), k.ggain[:, r], jnp.zeros((56, 128), F32)], axis=0).T
            k.wgu[r, 512:640] = (k.wgu[r, 512:640].astype(F32) + turned).astype(BF)

    def finish_input(b):
        total = sums["dn1", b]
        total.wait()

        def body(i):
            r = rows(i, 32, 32)
            own = pl.ds(pl.multiple_of(b * 512 + t * 128 + i * 32, 32), 32)
            local = pl.ds(pl.multiple_of(b * 128 + i * 32, 32), 32)
            grad, source = total.value(r), k.xall[own, :].astype(F32)
            scale = lax.rsqrt(jnp.mean(source * source, axis=-1, keepdims=True) + EPSILON)
            weighted = k.gains[0:1, :] * grad
            k.out_x[local, :] = (
                k.out_x[local, :]
                + scale * weighted
                - source * (scale * scale * scale) * jnp.mean(source * weighted, axis=-1, keepdims=True)
            )

        loop(4, body)
        total.drain()

    D, GU, A = ("d0", "d1"), ("g0", "g1", "u0", "u1"), ("a0", "a1")
    down = ring["d"]
    k.ggain[...] = jnp.zeros_like(k.ggain)
    gate_up(0)
    down.pump()
    ex["n2", 1].finish()
    gate_up(1)
    down.pump()
    down.pump()
    for b in range(MB):
        ex["dy", b].drain()
    grad_down()
    start(*D)
    for _ in range(4):
        down.pump()
    hidden_grads(0)
    pump(*D)
    second_norm_part(0)
    hidden_grads(1)
    pump(*D)
    sums["dn2", 0].middle()
    second_norm_part(1)
    for name in ("g", "u"):
        ring[name].drain()
    grad_gate_up()
    start(*GU)
    sums["dn2", 1].middle()
    pump(*D)
    finish_hidden_grad(0)
    pump(*D)
    finish_hidden_grad(1)
    pump(*D)
    ex["dh", 0].forward()
    pump(*GU)
    output_part(0)
    pump(*D)
    ex["dh", 1].forward()
    output_part(1)
    sums["out", 0].middle()
    pump(*D)
    for b in range(MB):
        ex["dh", b].finish()
    grad_out()
    start("o")
    sums["out", 1].middle()
    pump(*GU)
    mixed_grad()
    attend_back(0)
    finish_output(0)
    pump(*GU)
    pump("o")
    first_norm_part(0)
    for b in range(MB):
        ex["dh", b].drain()
    first_norm_again(0)
    finish_output(1)
    pump(*GU)
    sums["dn1", 0].middle()
    attend_back(1)
    pump(*GU)
    pump("o")
    first_norm_part(1)
    first_norm_again(1)
    grad_first()
    start(*A)
    sums["dn1", 1].middle()
    pump("o")
    pump(*GU)
    finish_input(0)
    pump(*A)
    pump("o")
    pump(*GU)
    pump(*A)
    pump("o")
    finish_input(1)
    pump(*A)
    pump("o")
    pump(*A)
    pump("o")
    pump(*A)
    pump(*A)
    pump(*A)

    part_rows = shard // 4
    for rank in range(4):
        here = slice(rank * part_rows, (rank + 1) * part_rows)
        k.kvsend[rank, :, 0:256] = k.out_a[here, 0:256]
        k.kvsend[rank, :, 256:384] = k.out_a[here, 512:640]
    tail = []
    for i, peer in enumerate((k.sib, k.far, cross)):
        tail.append(pltpu.make_async_remote_copy(
            k.kvsend.at[peer], k.out_kv.at[t], k.kv_s.at[3 + i], k.kv_r.at[3 + i], (f, peer), MESH))
    own = pltpu.make_async_copy(k.kvsend.at[t], k.out_kv.at[t], k.loc.at[9])
    own.start()
    for copy in tail:
        copy.start()
    for copy in tail:
        copy.wait_recv()
    own.wait()
    for copy in tail + kv_copies:
        copy.wait_send()
    for name in ("x", "n2"):
        for b in range(MB):
            ex[name, b].drain()
    for chunk in scatter.values():
        chunk.drain()


def layer(n, shard, arrays, debug=(), stop=None):
    def shape(dims, kind=BF):
        return jax.ShapeDtypeStruct(dims, kind)

    inputs = ("xin", "dyin", "apre", "kv4", "gate", "up", "down", "seg", "pos", "par", "freq")
    spaces = dict(xin=pl.ANY, dyin=pl.ANY, apre=pltpu.VMEM, kv4=pl.ANY, gate=pl.ANY, up=pl.ANY, down=pl.ANY,
                  seg=pltpu.VMEM, pos=pltpu.VMEM, par=pltpu.SMEM, freq=pltpu.VMEM)
    outputs = {
        "out_y": shape((256, 1280)),
        "out_x": shape((256, 1280), F32),
        "out_d": shape((shard, 896), F32),
        "out_g": shape((shard, 896), F32),
        "out_u": shape((shard, 896), F32),
        "out_a": shape((shard, AW), F32),
        "out_kv": shape((4, shard // 4, 384), F32),
    }
    half = shard // 2
    dma = pltpu.SemaphoreType.DMA
    scratch = {
        "wa": pltpu.VMEM((1280, AW), BF),
        "wgu": pltpu.VMEM((1280, 1792), BF),
        "wd": pltpu.VMEM((1280, 896), BF),
        "xall": pltpu.VMEM((1024, 1280), BF),
        "dyall": pltpu.VMEM((1024, 1280), BF),
        "n2all": pltpu.VMEM((1024, 1280), BF),
        "stage": pltpu.VMEM((shard, AW), BF),
        "kvr": pltpu.VMEM((4, shard // 4, 384), BF),
        "qkv": pltpu.VMEM((1024, QKV), BF),
        "kvrot": pltpu.VMEM((1024, 256), BF),
        "att": pltpu.VMEM((1024, 384), BF),
        "prob": pltpu.VMEM((10, 512, 512), BF),
        "bias": pltpu.VMEM((1024, 512), BF),
        "cs": pltpu.VMEM((1024, 256), F32),
        "gains": pltpu.VMEM((8, 1280), F32),
        "ggain": pltpu.VMEM((8, 1280), F32),
        "m": pltpu.VMEM((1024, 896), BF),
        "ab": pltpu.VMEM((1024, 1792), BF),
        "part": pltpu.VMEM((2, 2, 2, 128, 1280), BF),
        "near": pltpu.VMEM((2, 2, 2, 128, 1280), BF),
        "half": pltpu.VMEM((2, 2, 128, 1280), BF),
        "far_in": pltpu.VMEM((2, 2, 128, 1280), BF),
        "hid": pltpu.VMEM((256, 1280), F32),
        "gd": pltpu.VMEM((1280, 896), BF),
        "ggu": pltpu.VMEM((1280, 1792), BF),
        "slot_d": pltpu.VMEM((2, n - 1, half, 896), BF),
        "slot_gu": pltpu.VMEM((2, n - 1, half, 1792), BF),
        "slot_a": pltpu.VMEM((2, n - 1, half, AW), BF),
        "dq": pltpu.VMEM((512, 384), F32),
        "dkv": pltpu.VMEM((512, 256), F32),
        "kvsend": pltpu.VMEM((4, shard // 4, 384), F32),
        "loc": dma((10,)),
        "kv_s": dma((6,)), "kv_r": dma((6,)),
        "ex_s": dma((8, 3)), "ex_r": dma((8, 3)),
        "ts_s": dma((8, 2)), "ts_r": dma((8, 2)),
        "ga_s": dma((10, n - 1)), "ga_r": dma((10, n - 1)),
        "rs_s": dma((18, n - 1)), "rs_r": dma((18, n - 1)),
    }
    outs = dict(outputs)
    for name in debug:
        outs["dbg_" + name] = shape(scratch[name].shape, scratch[name].dtype)
    names = inputs + tuple(outs) + tuple(scratch)
    return pl.pallas_call(
        functools.partial(layer_kernel, n, shard, names, debug, stop),
        out_shape=tuple(outs.values()),
        in_specs=[pl.BlockSpec(memory_space=spaces[name]) for name in inputs],
        out_specs=tuple(
            pl.BlockSpec(memory_space=pl.ANY if name.startswith("dbg_") else pltpu.VMEM) for name in outs),
        scratch_shapes=list(scratch.values()),
        compiler_params=pltpu.CompilerParams(
            collective_id=0, has_side_effects=True, vmem_limit_bytes=67043328),
        name="layer",
    )(*arrays)


def fused_device(mesh_n, debug, stop, inputs, cotangent, segment_ids, parents, positions, norm1_gain, w_query, w_key,
                 w_value, w_out, norm2_gain, w_gate, w_up, w_down):
    shard = w_query.shape[0]
    apre = jnp.concatenate(
        [jnp.zeros((shard, 256), BF), w_query, jnp.zeros((shard, 64), BF), w_out.T, jnp.zeros((shard, 64), BF)], axis=1)
    quarter = shard // 4
    gain_lanes = jnp.concatenate(
        [jnp.zeros((quarter, 64), BF), norm1_gain[:, None], norm2_gain[:, None], jnp.zeros((quarter, 62), BF)], axis=1)
    kv4 = jnp.stack([
        jnp.concatenate([w_key[:, rank * 64:rank * 64 + 128], w_value[:, rank * 64:rank * 64 + 128], gain_lanes], axis=1)
        for rank in range(4)])
    steps = 1.0 / ROPE_BASE ** (jnp.arange(32, dtype=F32) / 32)
    freq = jnp.broadcast_to(jnp.tile(steps, 4)[None], (8, 128))
    outs = layer(mesh_n, shard, (
        inputs, cotangent, apre, kv4, w_gate, w_up, w_down.T, segment_ids, positions, parents, freq), debug, stop)
    y, gx, gd, gg, gu, ga, kv = outs[:7]
    key = sum(jnp.pad(kv[rank, :, 0:128], ((0, 0), (rank * 64, 192 - rank * 64))) for rank in range(4))
    value = sum(jnp.pad(kv[rank, :, 128:256], ((0, 0), (rank * 64, 192 - rank * 64))) for rank in range(4))
    gains = jnp.sum(kv[:, :, 320:322], axis=0)
    return (
        y.reshape(2, 128, 1280), gx.reshape(2, 128, 1280), gains[:, 0], ga[:, 256:576], key, value,
        ga[:, 640:960].T, gains[:, 1], gg, gu, gd.T) + tuple(outs[7:])


def across_rows(left_side, right_side):
    return lax.dot_general(
        left_side, right_side, (((0,), (0,)), ((), ())), preferred_element_type=jnp.float32
    )


def against_rows(left_side, right_side):
    return lax.dot_general(
        left_side, right_side, (((1,), (1,)), ((), ())), preferred_element_type=jnp.float32
    )


def norm_scale(values):
    return lax.rsqrt(jnp.mean(values * values, axis=-1, keepdims=True) + EPSILON)


def rotate(values, places, turning):
    half_width = HD // 2
    frequency = 1.0 / ROPE_BASE ** (jnp.arange(half_width, dtype=jnp.float32) / half_width)
    angles = places.astype(jnp.float32)[..., None] * frequency
    cosine = jnp.cos(angles)[..., None, :]
    sine_part = turning * jnp.sin(angles)[..., None, :]
    shaped = values.reshape(values.shape[:-1] + (values.shape[-1] // HD, HD))
    first_half = shaped[..., :half_width]
    second_half = shaped[..., half_width:]
    turned = jnp.concatenate(
        [
            first_half * cosine - second_half * sine_part,
            second_half * cosine + first_half * sine_part,
        ],
        axis=-1,
    )
    return turned.reshape(values.shape)


def lineage(segment, table):
    labels = jnp.arange(13, dtype=jnp.int32)
    first_label = jnp.min(segment) // 13 * 13
    picked = (segment - first_label)[:, None] == labels[None, :]
    parent = jnp.sum(jnp.where(picked, table[None, :], 0), axis=1)
    picked_two = (parent - first_label)[:, None] == labels[None, :]
    grand_parent = jnp.sum(jnp.where(picked_two, table[None, :], 0), axis=1)
    return (parent, grand_parent)


def allowed_pairs(block_segment, block_parent, block_grand, block_places, segment, places):
    same_path = (
        (segment[None, :] == block_segment[:, None])
        | (segment[None, :] == block_parent[:, None])
        | (segment[None, :] == block_grand[:, None])
    )
    return same_path & (places[None, :] <= block_places[:, None])


def rows_in(values):
    return lax.all_gather(values, "tp", axis=0, tiled=True)


def rows_out(term):
    return lax.psum_scatter(
        term.astype(jnp.bfloat16), "tp", scatter_dimension=0, tiled=True
    ).astype(jnp.float32)


def fetch_weights(w_query, w_out, w_key, w_value, norm1_gain, norm2_gain, w_gate, w_up, w_down):
    query_full, out_full = (
        lax.all_gather(w_query, "fsdp", axis=0, tiled=True),
        lax.all_gather(w_out, "fsdp", axis=1, tiled=True),
    )
    key_full, value_full, gain_one, gain_two = (
        lax.all_gather(w_key, ("fsdp", "tp"), axis=0, tiled=True),
        lax.all_gather(w_value, ("fsdp", "tp"), axis=0, tiled=True),
        lax.all_gather(norm1_gain, ("fsdp", "tp"), axis=0, tiled=True),
        lax.all_gather(norm2_gain, ("fsdp", "tp"), axis=0, tiled=True),
    )
    gate_full, up_full, down_full = (
        lax.all_gather(w_gate, "fsdp", axis=0, tiled=True),
        lax.all_gather(w_up, "fsdp", axis=0, tiled=True),
        lax.all_gather(w_down, "fsdp", axis=1, tiled=True),
    )
    return (
        query_full,
        key_full,
        value_full,
        out_full,
        gain_one.astype(jnp.float32),
        gain_two.astype(jnp.float32),
        gate_full,
        up_full,
        down_full,
    )


def reduce_grads(gradients):
    grad_q, grad_k, grad_v, grad_o, grad_g1, grad_g2, grad_gt, grad_u, grad_dn = gradients
    part_q, part_o, part_gt, part_u, part_dn = (
        lax.psum_scatter(grad_q, "fsdp", scatter_dimension=0, tiled=True),
        lax.psum_scatter(grad_o, "fsdp", scatter_dimension=1, tiled=True),
        lax.psum_scatter(grad_gt, "fsdp", scatter_dimension=0, tiled=True),
        lax.psum_scatter(grad_u, "fsdp", scatter_dimension=0, tiled=True),
        lax.psum_scatter(grad_dn, "fsdp", scatter_dimension=1, tiled=True),
    )
    part_k, part_v, part_g1, part_g2 = (
        lax.psum_scatter(grad_k, ("fsdp", "tp"), scatter_dimension=0, tiled=True),
        lax.psum_scatter(grad_v, ("fsdp", "tp"), scatter_dimension=0, tiled=True),
        lax.psum_scatter(grad_g1, ("fsdp", "tp"), scatter_dimension=0, tiled=True),
        lax.psum_scatter(grad_g2, ("fsdp", "tp"), scatter_dimension=0, tiled=True),
    )
    return (part_q, part_k, part_v, part_o, part_g1, part_g2, part_gt, part_u, part_dn)


def attention_forward(query_heads, keys_heads, values_heads, segment, parent, grand_parent, places):
    group_rows, local_heads = (query_heads.shape[0], query_heads.shape[1])
    block_rows = min(512, group_rows)
    block_count = group_rows // block_rows
    scale = HD ** (-0.5)

    def one_block(pieces):
        query_block, block_segment, block_parent, block_grand, block_places = pieces
        allowed = allowed_pairs(
            block_segment, block_parent, block_grand, block_places, segment, places
        )
        scores = (
            jnp.einsum("qhd,khd->hqk", query_block, keys_heads, preferred_element_type=jnp.float32)
            * scale
        )
        scores = jnp.where(allowed[None], scores, MASKED)
        row_peak = jnp.max(scores, axis=-1, keepdims=True)
        weights_row = jnp.exp(scores - row_peak)
        row_total = jnp.sum(weights_row, axis=-1, keepdims=True)
        probability = weights_row / row_total
        mixed = jnp.einsum(
            "hqk,khd->qhd",
            probability.astype(jnp.bfloat16),
            values_heads,
            preferred_element_type=jnp.float32,
        )
        return (mixed.astype(jnp.bfloat16), (row_peak + jnp.log(row_total))[..., 0])

    pieces = (
        query_heads.reshape(block_count, block_rows, local_heads, HD),
        segment.reshape(block_count, block_rows),
        parent.reshape(block_count, block_rows),
        grand_parent.reshape(block_count, block_rows),
        places.reshape(block_count, block_rows),
    )
    mixed, log_total = lax.map(one_block, pieces)
    return (mixed.reshape(group_rows, local_heads * HD), log_total)


def attention_backward(
    query_heads,
    keys_heads,
    values_heads,
    grad_mixed,
    log_total,
    segment,
    parent,
    grand_parent,
    places,
):
    group_rows, local_heads = (query_heads.shape[0], query_heads.shape[1])
    block_rows = min(512, group_rows)
    block_count = group_rows // block_rows
    scale = HD ** (-0.5)

    def one_block(running, pieces):
        key_grad, value_grad = running
        (
            query_block,
            out_block,
            block_log,
            block_segment,
            block_parent,
            block_grand,
            block_places,
        ) = pieces
        allowed = allowed_pairs(
            block_segment, block_parent, block_grand, block_places, segment, places
        )
        scores = (
            jnp.einsum("qhd,khd->hqk", query_block, keys_heads, preferred_element_type=jnp.float32)
            * scale
        )
        probability = jnp.where(allowed[None], jnp.exp(scores - block_log[..., None]), 0.0)
        grad_prob = jnp.einsum(
            "qhd,khd->hqk", out_block, values_heads, preferred_element_type=jnp.float32
        )
        row_delta = jnp.sum(probability * grad_prob, axis=-1, keepdims=True)
        grad_score = (scale * probability * (grad_prob - row_delta)).astype(jnp.bfloat16)
        query_grad = jnp.einsum(
            "hqk,khd->qhd", grad_score, keys_heads, preferred_element_type=jnp.float32
        )
        key_grad = key_grad + jnp.einsum(
            "hqk,qhd->khd", grad_score, query_block, preferred_element_type=jnp.float32
        )
        value_grad = value_grad + jnp.einsum(
            "hqk,qhd->khd",
            probability.astype(jnp.bfloat16),
            out_block,
            preferred_element_type=jnp.float32,
        )
        return ((key_grad, value_grad), query_grad)

    zeros_heads = jnp.zeros((group_rows, local_heads, HD), jnp.float32)
    pieces = (
        query_heads.reshape(block_count, block_rows, local_heads, HD),
        grad_mixed.reshape(block_count, block_rows, local_heads, HD),
        log_total,
        segment.reshape(block_count, block_rows),
        parent.reshape(block_count, block_rows),
        grand_parent.reshape(block_count, block_rows),
        places.reshape(block_count, block_rows),
    )
    (key_grad, value_grad), query_grad = lax.scan(one_block, (zeros_heads, zeros_heads), pieces)
    return (query_grad.reshape(group_rows, local_heads, HD), key_grad, value_grad)


def per_device(
    inputs,
    cotangent,
    segment_ids,
    parents,
    positions,
    norm1_gain,
    w_query,
    w_key,
    w_value,
    w_out,
    norm2_gain,
    w_gate,
    w_up,
    w_down,
):
    head_rank = lax.axis_index("tp")
    local_heads = w_query.shape[1] // HD
    key_head = (head_rank * local_heads + jnp.arange(local_heads, dtype=jnp.int32)) // (H // KV)
    head_choice = (key_head[:, None] == jnp.arange(KV, dtype=jnp.int32)[None, :]).astype(
        jnp.float32
    )
    choice_low = head_choice.astype(jnp.bfloat16)
    outputs = []
    input_grads = []
    shards = None
    for batch_index in range(MB):
        weights = fetch_weights(
            w_query, w_out, w_key, w_value, norm1_gain, norm2_gain, w_gate, w_up, w_down
        )
        (
            query_full,
            key_full,
            value_full,
            out_full,
            gain_one,
            gain_two,
            gate_full,
            up_full,
            down_full,
        ) = weights
        source = inputs[batch_index].astype(jnp.float32)
        segment = segment_ids[batch_index]
        places = positions[batch_index]
        parent, grand_parent = lineage(segment, parents[batch_index])
        norm_one = norm_scale(source)
        normed = (source * norm_one * gain_one).astype(jnp.bfloat16)
        normed_all = rows_in(normed)
        queries = rotate(
            jnp.dot(normed_all, query_full, preferred_element_type=jnp.float32), places, 1.0
        ).astype(jnp.bfloat16)
        keys_all = rotate(
            jnp.dot(normed_all, key_full, preferred_element_type=jnp.float32), places, 1.0
        ).astype(jnp.bfloat16)
        values_all = jnp.dot(normed_all, value_full, preferred_element_type=jnp.float32).astype(
            jnp.bfloat16
        )
        group_rows = keys_all.shape[0]
        keys_heads = jnp.einsum(
            "gkd,hk->ghd",
            keys_all.reshape(group_rows, KV, HD),
            choice_low,
            preferred_element_type=jnp.float32,
        ).astype(jnp.bfloat16)
        values_heads = jnp.einsum(
            "gkd,hk->ghd",
            values_all.reshape(group_rows, KV, HD),
            choice_low,
            preferred_element_type=jnp.float32,
        ).astype(jnp.bfloat16)
        query_heads = queries.reshape(group_rows, local_heads, HD)
        attended, log_total = attention_forward(
            query_heads, keys_heads, values_heads, segment, parent, grand_parent, places
        )
        hidden = source + rows_out(jnp.dot(attended, out_full, preferred_element_type=jnp.float32))
        norm_two = norm_scale(hidden)
        normed_two = (hidden * norm_two * gain_two).astype(jnp.bfloat16)
        normed_two_all = rows_in(normed_two)
        gate_pre = jnp.dot(normed_two_all, gate_full, preferred_element_type=jnp.float32)
        upward = jnp.dot(normed_two_all, up_full, preferred_element_type=jnp.float32)
        sigmoid_gate = jax.nn.sigmoid(gate_pre)
        activated = gate_pre * sigmoid_gate
        product = (activated * upward).astype(jnp.bfloat16)
        output = hidden + rows_out(jnp.dot(product, down_full, preferred_element_type=jnp.float32))
        grad_hidden = cotangent[batch_index].astype(jnp.float32)
        grad_branch = rows_in(grad_hidden.astype(jnp.bfloat16))
        grad_product = against_rows(grad_branch, down_full)
        grad_down_w = across_rows(product, grad_branch)
        grad_gate_pre = (
            grad_product * upward * sigmoid_gate * (1.0 + gate_pre * (1.0 - sigmoid_gate))
        ).astype(jnp.bfloat16)
        grad_upward = (grad_product * activated).astype(jnp.bfloat16)
        grad_gate_w = across_rows(normed_two_all, grad_gate_pre)
        grad_up_w = across_rows(normed_two_all, grad_upward)
        grad_normed_two = rows_out(
            against_rows(grad_gate_pre, gate_full) + against_rows(grad_upward, up_full)
        )
        gain_two_grad = jnp.sum(hidden * norm_two * grad_normed_two, axis=0)
        weighted_two = gain_two * grad_normed_two
        grad_hidden = (
            grad_hidden
            + norm_two * weighted_two
            - hidden
            * (norm_two * norm_two * norm_two)
            * jnp.mean(hidden * weighted_two, axis=-1, keepdims=True)
        )
        grad_attn = rows_in(grad_hidden.astype(jnp.bfloat16))
        grad_out_w = across_rows(attended, grad_attn)
        grad_mixed = (
            against_rows(grad_attn, out_full)
            .astype(jnp.bfloat16)
            .reshape(group_rows, local_heads, HD)
        )
        query_grad, key_grad, value_grad = attention_backward(
            query_heads,
            keys_heads,
            values_heads,
            grad_mixed,
            log_total,
            segment,
            parent,
            grand_parent,
            places,
        )
        key_part = jnp.einsum(
            "ghd,hk->gkd", key_grad, head_choice, precision=lax.Precision.HIGHEST
        ).reshape(group_rows, KV * HD)
        value_part = jnp.einsum(
            "ghd,hk->gkd", value_grad, head_choice, precision=lax.Precision.HIGHEST
        ).reshape(group_rows, KV * HD)
        key_part = rotate(key_part, places, -1.0)
        query_raw = rotate(query_grad.reshape(group_rows, local_heads * HD), places, -1.0).astype(
            jnp.bfloat16
        )
        grad_query_w = across_rows(normed_all, query_raw)
        normed_term = against_rows(query_raw, query_full)
        grad_normed = lax.psum_scatter(
            normed_term.astype(jnp.bfloat16), "tp", scatter_dimension=0, tiled=True
        ).astype(jnp.float32)
        key_sum = lax.psum_scatter(
            key_part.astype(jnp.bfloat16), "tp", scatter_dimension=0, tiled=True
        )
        value_sum = lax.psum_scatter(
            value_part.astype(jnp.bfloat16), "tp", scatter_dimension=0, tiled=True
        )
        grad_key_w = across_rows(normed, key_sum)
        grad_value_w = across_rows(normed, value_sum)
        grad_normed = (
            grad_normed + against_rows(key_sum, key_full) + against_rows(value_sum, value_full)
        )
        gain_one_grad = jnp.sum(source * norm_one * grad_normed, axis=0)
        weighted_one = gain_one * grad_normed
        grad_source = (
            grad_hidden
            + norm_one * weighted_one
            - source
            * (norm_one * norm_one * norm_one)
            * jnp.mean(source * weighted_one, axis=-1, keepdims=True)
        )
        gradients = (
            grad_query_w,
            grad_key_w,
            grad_value_w,
            grad_out_w,
            gain_one_grad,
            gain_two_grad,
            grad_gate_w,
            grad_up_w,
            grad_down_w,
        )
        output, grad_source, gradients = (output.astype(jnp.bfloat16), grad_source, gradients)
        outputs.append(output)
        input_grads.append(grad_source)
        summed = reduce_grads(gradients)
        shards = summed if batch_index == 0 else jax.tree.map(jnp.add, shards, summed)
    return (
        jnp.stack(outputs),
        jnp.stack(input_grads),
        shards[4],
        shards[0],
        shards[1],
        shards[2],
        shards[3],
        shards[5],
        shards[6],
        shards[7],
        shards[8],
    )


def solution(mesh):
    placed = (
        P(None, ("fsdp", "tp"), None),
        P(None, ("fsdp", "tp"), None),
        P(None, "fsdp"),
        P(None, "fsdp"),
        P(None, "fsdp"),
        P(("fsdp", "tp")),
        P("fsdp", "tp"),
        P(("fsdp", "tp"), None),
        P(("fsdp", "tp"), None),
        P("tp", "fsdp"),
        P(("fsdp", "tp")),
        P("fsdp", "tp"),
        P("fsdp", "tp"),
        P("tp", "fsdp"),
    )
    ring = mesh.shape["fsdp"]
    body = functools.partial(fused_device, ring, (), None) if ring == 8 else per_device
    return jax.shard_map(
        body,
        mesh=mesh,
        in_specs=placed,
        out_specs=(
            P(None, ("fsdp", "tp"), None),
            P(None, ("fsdp", "tp"), None),
            P(("fsdp", "tp")),
            P("fsdp", "tp"),
            P(("fsdp", "tp"), None),
            P(("fsdp", "tp"), None),
            P("tp", "fsdp"),
            P(("fsdp", "tp")),
            P("fsdp", "tp"),
            P("fsdp", "tp"),
            P("tp", "fsdp"),
        ),
        check_vma=False,
    )
```

```python
import functools
import types

import jax
import jax.numpy as jnp
import numpy as np
from jax import lax
from jax.experimental import pallas as pl
from jax.experimental.pallas import tpu as pltpu
from jax.sharding import PartitionSpec as P

EPSILON = 1e-05
ROPE_BASE = 10000.0
MASKED = -1e30
H = 20
KV = 5
HD = 64
MB = 2
MESH = pl.DeviceIdType.MESH
BF = jnp.bfloat16
F32 = jnp.float32
QKV = 640
AW = 1024
SPANS = ((0, 512), (512, 896))
WF = ((0, 512, 1024, 1536), (1536, 1920, 2304, 2688))
AB = ((0, 512, 1024), (1024, 1408, 1792))


def dot(left, right, left_dim, right_dim):
    return lax.dot_general(
        left, right, (((left_dim,), (right_dim,)), ((), ())), preferred_element_type=F32
    )


def loop(count, body):
    def step(index, carry):
        body(index)
        return carry

    lax.fori_loop(0, count, step, 0)


def rows(index, size, extent):
    return pl.ds(pl.multiple_of(index * size, size), extent)


def swap_halves(values):
    lane = lax.broadcasted_iota(jnp.int32, values.shape, 1)
    return jnp.where(lane % 64 < 32, pltpu.roll(values, 96, 1), pltpu.roll(values, 32, 1))


class Exchange:
    def __init__(self, k, tag, whole, base, source=None):
        own, near, far = k.t, k.x * 2 + 1 - k.c, (1 - k.x) * 2 + k.c
        self.whole = whole

        def block(rank):
            return whole.at[pl.ds(pl.multiple_of(base + rank * 128, 128), 128)]

        src = block(own) if source is None else source
        self.to_sib = pltpu.make_async_remote_copy(
            src, block(own), k.ex_s.at[tag, 0], k.ex_r.at[tag, 0], (k.f, k.sib), MESH)
        self.to_far = pltpu.make_async_remote_copy(
            src, block(own), k.ex_s.at[tag, 1], k.ex_r.at[tag, 1], (k.f, k.far), MESH)
        self.relay = pltpu.make_async_remote_copy(
            block(far), block(far), k.ex_s.at[tag, 2], k.ex_r.at[tag, 2], (k.f, k.sib), MESH)

    def start(self):
        self.to_far.start()
        self.to_sib.start()

    def forward(self):
        self.to_far.wait_recv()
        self.relay.start()

    def finish(self):
        self.to_sib.wait_recv()
        self.relay.wait_recv()

    def drain(self):
        self.to_far.wait_send()
        self.to_sib.wait_send()
        self.relay.wait_send()


class TreeSum:
    def __init__(self, k, tag, keep, b):
        self.k, self.b, self.keep = k, b, keep
        self.inner = pltpu.make_async_remote_copy(
            k.part.at[b, 1 - k.c], k.near.at[keep, b], k.ts_s.at[tag, 0], k.ts_r.at[tag, 0], (k.f, k.sib), MESH)
        self.outer = pltpu.make_async_remote_copy(
            k.half.at[keep, b], k.far_in.at[keep, b], k.ts_s.at[tag, 1], k.ts_r.at[tag, 1], (k.f, k.far), MESH)

    def start(self):
        self.inner.start()

    def middle(self):
        k, b, keep = self.k, self.b, self.keep
        self.inner.wait_recv()
        other = 1 - k.x

        def body(i):
            r = rows(i, 32, 32)
            k.half[keep, b, r, :] = (
                k.part[b, k.c, other, r, :].astype(F32) + k.near[keep, b, other, r, :].astype(F32)
            ).astype(BF)

        loop(4, body)
        self.outer.start()

    def wait(self):
        self.outer.wait_recv()

    def value(self, r):
        k, b, keep = self.k, self.b, self.keep
        return (
            k.part[b, k.c, k.x, r, :].astype(F32)
            + k.near[keep, b, k.x, r, :].astype(F32)
            + k.far_in[keep, b, r, :].astype(F32)
        )

    def drain(self):
        self.inner.wait_send()
        self.outer.wait_send()


class RingGather:
    def __init__(self, k, tag, whole, lane, width):
        self.k, self.tag, self.whole, self.lane, self.width = k, tag, whole, lane, width
        self.step = 0

    def copy(self, way, s):
        k = self.k
        first, half = k.first[(k.n - s if way == 0 else s) % k.n], k.shard // 2
        if s < k.n // 2 - 1:
            where = pl.ds(pl.multiple_of(first, 16), k.shard)
        else:
            where = pl.ds(pl.multiple_of(first + way * half, 16), half)
        ref = self.whole.at[where, pl.ds(self.lane, self.width)]
        return pltpu.make_async_remote_copy(
            ref, ref, k.ga_s.at[self.tag * 2 + way, s], k.ga_r.at[self.tag * 2 + way, s],
            (k.next if way == 0 else k.prev, k.t), MESH)

    def start(self):
        for way in (0, 1):
            self.copy(way, 0).start()

    def pump(self):
        s = self.step
        self.step += 1
        for way in (0, 1):
            self.copy(way, s).wait_recv()
            if s < self.k.n // 2 - 1:
                self.copy(way, s + 1).start()

    def drain(self):
        if self.step:
            self.step = 0
            for s in range(self.k.n // 2):
                for way in (0, 1):
                    self.copy(way, s).wait_send()


class RingSum:
    def __init__(self, k, tag, grad, lane, width, slots, slot_lane, result, out_lane):
        self.k, self.tag, self.grad, self.lane, self.width = k, tag, grad, lane, width
        self.slots, self.slot_lane, self.result, self.out_lane = slots, slot_lane, result, out_lane
        self.step = 0

    def first_row(self, way, long, away):
        k = self.k
        part = way if long else 1 - way
        return pl.multiple_of(k.first[(away if way == 0 else k.n - away) % k.n] + part * (k.shard // 2), 16)

    def copy(self, way, long, s):
        k = self.k
        hops = k.n // 2 if long else k.n // 2 - 1
        base = 0 if long else k.n // 2
        lanes = pl.ds(self.slot_lane, self.width)
        if s == 0:
            src = self.grad.at[pl.ds(self.first_row(way, long, hops), k.shard // 2), pl.ds(self.lane, self.width)]
        else:
            src = self.slots.at[way, base + s - 1, :, lanes]
        return pltpu.make_async_remote_copy(
            src, self.slots.at[way, base + s, :, lanes],
            k.rs_s.at[self.tag * 2 + way, base + s], k.rs_r.at[self.tag * 2 + way, base + s],
            (k.next if way == 0 else k.prev, k.t), MESH)

    def start(self):
        for long in (True, False):
            for way in (0, 1):
                self.copy(way, long, 0).start()

    def pump(self):
        k, s = self.k, self.step
        self.step += 1
        half = k.shard // 2
        lanes, slot_lanes = pl.ds(self.lane, self.width), pl.ds(self.slot_lane, self.width)
        out_lanes = pl.ds(self.out_lane, self.width)
        for long in (True, False):
            hops = k.n // 2 if long else k.n // 2 - 1
            for way in (0, 1):
                if s >= hops:
                    continue
                self.copy(way, long, s).wait_recv()
                slot = s if long else k.n // 2 + s
                first = self.first_row(way, long, hops - 1 - s)
                out = (way if long else 1 - way) * half

                def body(i):
                    r = rows(i, 16, 16)
                    total = self.slots[way, slot, r, slot_lanes].astype(F32)
                    there = pl.ds(pl.multiple_of(out + i * 16, 16), 16)
                    if long and s == hops - 1:
                        self.result[there, out_lanes] += total
                        return
                    total += self.grad[pl.ds(pl.multiple_of(first + i * 16, 16), 16), lanes].astype(F32)
                    if s < hops - 1:
                        self.slots[way, slot, r, slot_lanes] = total.astype(BF)
                    else:
                        self.result[there, out_lanes] = total

                loop(half // 16, body)
                if s < hops - 1:
                    self.copy(way, long, s + 1).start()

    def drain(self):
        for long in (True, False):
            for s in range(self.k.n // 2 if long else self.k.n // 2 - 1):
                for way in (0, 1):
                    self.copy(way, long, s).wait_send()


class Kernel:
    pass


def order(o):
    o.tab1(); o.o(); o.tab0(); o.xf(); o.dys(); o.kvq(); o.xd(); o.o(); o.su1(); o.kvq(); o.dyf(); o.kvq(); o.o()
    o.dyd(); o.sg1(); o.kvq(); o.u1(); o.gain(); o.su0(); o.pr1(); o.sd0(); o.o(); o.at1(); o.u1(); o.hp1(); o.u0()
    o.pr0(); o.g0(); o.at0(); o.hm1(); o.u1(); o.hp0(); o.u0(); o.g0(); o.u1(); o.hm0(); o.g1(); o.fh1(); o.u0()
    o.g0(); o.sd1(); o.fh0(); o.u0(); o.g1(); o.g0(); o.d0(); o.d1(); o.nf1(); o.g1(); o.nd1(); o.d0(); o.gu01()
    o.nf0(); o.d1(); o.g1(); o.gu11(); o.nd0(); o.gu10(); o.d0(); o.gu00(); o.d1(); o.gd0(); o.d0(); o.hg00()
    o.gd1(); o.d1(); o.hg10(); o.sn0(); o.rd0(); o.hg11(); o.gg1(); o.hg01(); o.dm0(); o.sn1(); o.rd0(); o.gg0()
    o.dm1(); o.fd0(); o.yp0(); o.rd0(); o.re0(); o.ym0(); o.fd1(); o.yp1(); o.rd0(); o.rd1(); o.df0(); o.ym1()
    o.re0(); o.dd0(); o.mg0(); o.rd1(); o.re1(); o.ba0(); o.df1(); o.fy0(); o.fp0(); o.re0(); o.fg0(); o.dd1()
    o.rd1(); o.go(); o.im0(); o.fy1(); o.cy(); o.mg1(); o.re1(); o.ba1(); o.re0(); o.ro(); o.rd1(); o.fp1(); o.re1()
    o.na0(); o.na1(); o.ro(); o.gf(); o.re1(); o.cf(); o.im1(); o.fg1(); o.ro(); o.gl(); o.fi0(); o.ra0(); o.ro()
    o.ra1(); o.ra0(); o.fi1(); o.cx(); o.ra1(); o.ra0(); o.ra1(); o.ra0(); o.ra1()


def layer_kernel(n, shard, names, *refs):
    k = Kernel()
    for name, ref in zip(names, refs):
        setattr(k, name, ref)
    k.n, k.shard = n, shard
    f, t = lax.axis_index("fsdp"), lax.axis_index("tp")
    k.f, k.t, k.x, k.c = f, t, t // 2, t % 2
    k.sib = k.x * 2 + 1 - k.c
    k.far = (1 - k.x) * 2 + k.c
    cross = (1 - k.x) * 2 + 1 - k.c
    even = 1 - f % 2
    k.p = even * (f // 2) + (1 - even) * (n - 1 - f // 2)

    def at_ring(place):
        high = place // (n // 2)
        return (1 - high) * (2 * place) + high * (2 * (n - 1 - place) + 1)

    spots = [at_ring((k.p + i) % n) for i in range(n)]
    k.first = [spot * shard for spot in spots]
    k.next, k.prev = spots[1], spots[n - 1]

    barrier = pltpu.get_barrier_semaphore()
    for peer in ((f, k.sib), (f, k.far), (f, cross), (k.next, t), (k.prev, t)):
        pl.semaphore_signal(barrier, inc=1, device_id=peer, device_id_type=MESH)

    part_rows = shard // 4
    k.ab[0:shard, QKV:QKV + 256] = k.wo[:, 0:256]
    k.ab[0:shard, QKV + 256:AW] = jnp.concatenate(
        [k.wo[:, 256:320].astype(F32), jnp.zeros((shard, 64), F32)], axis=1).astype(BF)
    columns = jnp.concatenate(
        [jnp.concatenate([k.gn[...], jnp.zeros((2, 128 - part_rows), F32)], axis=1), jnp.zeros((126, 128), F32)], axis=0).T
    gain_lanes = pltpu.roll(columns, 64, 1)[0:part_rows]
    wide_keys, wide_values = k.wk[...].astype(F32), k.wv[...].astype(F32)
    for rank in range(4):
        there = slice(256 + 48 * rank, 256 + 48 * rank + part_rows)
        k.ab[there, 0:128] = wide_keys[:, rank * 64:rank * 64 + 128].astype(BF)
        k.ab[there, 128:256] = wide_values[:, rank * 64:rank * 64 + 128].astype(BF)
        k.ab[there, 256:384] = gain_lanes.astype(BF)

    def kv_block(rank):
        return k.ab.at[pl.ds(pl.multiple_of(256 + 48 * rank, 16), part_rows), pl.ds(0, 384)]

    mine = pl.ds(pl.multiple_of(f * shard, 16), shard)
    locals_ = [
        pltpu.make_async_copy(
            k.ab.at[pl.ds(0, shard), pl.ds(QKV, AW - QKV)], k.wa.at[mine, pl.ds(QKV, AW - QKV)], k.loc.at[0]),
    ]
    for c in range(2):
        for i, whole in enumerate((k.gate, k.up, k.down)):
            low, high = SPANS[c]
            locals_.append(pltpu.make_async_copy(
                whole.at[:, pl.ds(low, high - low)], k.wf.at[mine, pl.ds(WF[c][i], high - low)], k.loc.at[10 + 3 * c + i]))
    token_copies = []
    for b in range(MB):
        own = pl.ds(pl.multiple_of(b * 512 + t * 128, 128), 128)
        token_copies.append(pltpu.make_async_copy(k.xin.at[b], k.xall.at[own], k.loc.at[3 + b]))
        token_copies.append(pltpu.make_async_copy(k.dyin.at[b], k.dyall.at[own], k.loc.at[5 + b]))
    for copy in locals_ + token_copies:
        copy.start()
    pl.semaphore_wait(barrier, 5)

    kv_copies = []
    for i, peer in enumerate((k.sib, k.far, cross)):
        kv_copies.append(pltpu.make_async_remote_copy(
            kv_block(peer), k.kvr.at[t], k.kv_s.at[i], k.kv_r.at[i], (f, peer), MESH))
    own_kv = pltpu.make_async_copy(kv_block(t), k.kvr.at[t], k.loc.at[7])
    own_kv.start()
    for copy in kv_copies:
        copy.start()
    ex = {}
    for b in range(MB):
        ex["x", b] = Exchange(k, b, k.xall, b * 512, k.xin.at[b])
        ex["dy", b] = Exchange(k, 2 + b, k.dyall, b * 512, k.dyin.at[b])
        ex["n2", b] = Exchange(k, 4 + b, k.n2all, b * 512)
        ex["dh", b] = Exchange(k, 6 + b, k.dyall, b * 512)
    for b in range(MB):
        ex["x", b].start()
    ring = {
        "kvq": RingGather(k, 0, k.wa, 0, 640),
        "o": RingGather(k, 1, k.wa, 640, 384),
    }
    for i in range(6):
        low, high = WF[i // 3][i % 3], WF[i // 3][i % 3 + 1]
        ring["gud"[i % 3] + str(i // 3)] = RingGather(k, 2 + i, k.wf, low, high - low)
    for copy in locals_:
        copy.wait()
    for name in ("o", "g0"):
        ring[name].start()
    for copy in kv_copies:
        copy.wait()
    own_kv.wait()

    for rank in range(4):
        here = slice(rank * part_rows, (rank + 1) * part_rows)
        k.ab[here, 0:256] = k.kvr[rank, :, 0:256]
        k.ab[here, 256:512] = k.wq[here, 0:256]
        k.ab[here, 512:640] = (jnp.concatenate(
            [k.wq[here, 256:320].astype(F32), jnp.zeros((part_rows, 64), F32)], axis=1)
            + k.kvr[rank, :, 256:384].astype(F32)).astype(BF)
    to_wa = pltpu.make_async_copy(k.ab.at[pl.ds(0, shard), pl.ds(0, QKV)], k.wa.at[mine, pl.ds(0, QKV)], k.loc.at[8])
    to_wa.start()
    to_wa.wait()
    ring["kvq"].start()
    lane = lax.broadcasted_iota(jnp.int32, (8, 128), 1)[0:1]

    def tables(b):
        stacked = jnp.concatenate(
            [k.seg[b:b + 1].astype(F32), k.pos[b:b + 1].astype(F32), jnp.zeros((126, 512), F32)], axis=0)
        columns = stacked.T
        seg_col, pos_col = columns[:, 0:1], columns[:, 1:2]
        first = (f * 13).astype(F32)
        parent = jnp.zeros((512, 1), F32)
        for label in range(13):
            parent = jnp.where(seg_col == first + label, k.par[b, label].astype(F32), parent)
        grand = jnp.zeros((512, 1), F32)
        for label in range(13):
            grand = jnp.where(parent == first + label, k.par[b, label].astype(F32), grand)
        seg_row, pos_row = stacked[0:1], stacked[1:2]
        for i in range(4):
            r = slice(i * 128, (i + 1) * 128)
            same = (
                (seg_row == seg_col[r]) | (seg_row == parent[r]) | (seg_row == grand[r])
            ) & (pos_row <= pos_col[r])
            k.bias[b * 512 + i * 128:b * 512 + (i + 1) * 128, :] = jnp.where(same, 0.0, MASKED).astype(BF)
            angle = pos_col[r] * k.freq[0:1, :]
            sign = jnp.where(lane % 64 < 32, -1.0, 1.0)
            k.cs[b * 512 + i * 128:b * 512 + (i + 1) * 128, 0:128] = jnp.cos(angle)
            k.cs[b * 512 + i * 128:b * 512 + (i + 1) * 128, 128:256] = jnp.sin(angle) * sign

    def tokens_in():
        for copy in token_copies:
            copy.wait()
        for b in range(MB):
            ex["x", b].finish()

    def gain_rows():
        for i in range(10):
            turned = k.wa[i * 128:(i + 1) * 128, 512:640].astype(F32).T
            k.gains[:, i * 128:(i + 1) * 128] = turned[64:72]

    def normed(r):
        source = k.xall[r, :].astype(F32)
        scale = lax.rsqrt(jnp.mean(source * source, axis=-1, keepdims=True) + EPSILON)
        return source * scale

    def project(b):
        def norm(i):
            k.n2all[rows(i, 64, 64), :] = (normed(pl.ds(pl.multiple_of(b * 512 + i * 64, 64), 64)) * k.gains[0:1, :]).astype(BF)

        loop(8, norm)

        def body(i):
            r = pl.ds(pl.multiple_of(b * 512 + i * 256, 256), 256)
            out = dot(k.n2all[rows(i, 256, 256), :], k.wa[:, 0:QKV], 1, 0)
            cos, sin = k.cs[r, 0:128], k.cs[r, 128:256]
            key = out[:, 0:128]
            key = key * cos + swap_halves(key) * sin
            value = out[:, 128:256]
            k.qkv[r, 0:128] = key.astype(BF)
            k.kvrot[r, 0:128] = pltpu.roll(key, 64, 1).astype(BF)
            k.qkv[r, 128:256] = value.astype(BF)
            k.kvrot[r, 128:256] = pltpu.roll(value, 64, 1).astype(BF)
            for chunk in range(3):
                u = out[:, 256 + chunk * 128:384 + chunk * 128]
                u = (u * cos + swap_halves(u) * sin) * HD ** (-0.5)
                if chunk == 2:
                    u = jnp.where(lax.broadcasted_iota(jnp.int32, u.shape, 1) < 64, u, 0.0)
                k.qkv[r, 256 + chunk * 128:384 + chunk * 128] = u.astype(BF)

        loop(2, body)

    def head_masks(h):
        parity = h % 2
        group = jnp.where(h < 4 - t, 0, 1)
        in_half = (lane // 64 == parity).astype(F32)
        straight = (group == parity).astype(F32)
        return parity, group, in_half, straight

    def pick(b, h, lanes):
        parity, group, in_half, straight = head_masks(h)
        r = slice(b * 512, (b + 1) * 512)
        keep = (in_half * straight).astype(BF)
        turn = (in_half * (1.0 - straight)).astype(BF)
        return k.qkv[r, lanes] * keep + k.kvrot[r, lanes] * turn

    def chunk_of(h, base):
        return pl.ds(pl.multiple_of(base + (h // 2) * 128, 128), 128)

    def attend(b):
        base = b * 512

        def head(h):
            keys, values = pick(b, h, slice(0, 128)), pick(b, h, slice(128, 256))
            q = k.qkv[base:base + 512, chunk_of(h, 256)]
            for low, high, width in ((0, 128, 128), (128, 512, 512)):
                s = dot(q[low:high], keys[0:width], 1, 1) + k.bias[base + low:base + high, 0:width].astype(F32)
                e = jnp.exp(s - jnp.max(s, axis=-1, keepdims=True))
                prob = (e / jnp.sum(e, axis=-1, keepdims=True)).astype(BF)
                k.prob[b * 5 + h, low:high, 0:width] = prob
                out = dot(prob, values[0:width], 1, 0)
                old = k.att[base + low:base + high, chunk_of(h, 0)].astype(F32)
                k.att[base + low:base + high, chunk_of(h, 0)] = (jnp.where(h % 2 == 1, old, 0.0) + out).astype(BF)

        loop(5, head)

    def put_part(b, i, value):
        for c in range(2):
            k.part[b, c, i] = value[c * 128:(c + 1) * 128].astype(BF)

    def two_blocks(b, body):
        def step(i):
            r = pl.ds(pl.multiple_of(b * 512 + i * 256, 256), 256)
            put_part(b, i, body(r))

        loop(2, step)

    sums = {}

    def tree_sum(name, tag, keep, b):
        sums[name, b] = TreeSum(k, tag + b, keep, b)
        sums[name, b].start()

    def out_proj(b):
        two_blocks(b, lambda r: dot(k.att[r, :], k.wa[:, QKV:AW], 1, 1))
        tree_sum("hid", 0, 0, b)

    def finish_hidden(b):
        sums["hid", b].wait()

        def body(i):
            r = rows(i, 32, 32)
            own = pl.ds(pl.multiple_of(b * 512 + t * 128 + i * 32, 32), 32)
            hid = k.xall[own, :].astype(F32) + sums["hid", b].value(r)
            k.hid[pl.ds(pl.multiple_of(b * 128 + i * 32, 32), 32), :] = hid
            scale = lax.rsqrt(jnp.mean(hid * hid, axis=-1, keepdims=True) + EPSILON)
            k.n2all[own, :] = (hid * scale * k.gains[1:2, :]).astype(BF)

        loop(4, body)
        ex["n2", b].start()
        sums["hid", b].drain()

    ops = {"xf": lambda: [ex["x", b].forward() for b in range(MB)], "xd": tokens_in, "gain": gain_rows,
           "dys": lambda: [ex["dy", b].start() for b in range(MB)],
           "dyf": lambda: [ex["dy", b].forward() for b in range(MB)],
           "dyd": lambda: [ex["dy", b].finish() for b in range(MB)]}
    for name, piece in ring.items():
        ops["s" + name], ops[name] = piece.start, piece.pump

    def each(name, body):
        for b in range(MB):
            ops[name + str(b)] = functools.partial(body, b)

    each("tab", tables)
    each("pr", project)
    each("at", attend)
    each("hp", out_proj)
    each("hm", lambda b: sums["hid", b].middle())
    each("fh", finish_hidden)
    each("nf", lambda b: ex["n2", b].forward())
    each("nd", lambda b: ex["n2", b].finish())
    scatter = backward(k, ex, ring, sums, tree_sum, two_blocks, normed, pick, head_masks, chunk_of, ops, each)
    k.ggain[...] = jnp.zeros_like(k.ggain)
    outs = {name: pltpu.make_async_copy(source, whole, k.loc.at[i]) for i, (name, source, whole) in enumerate(
        (("cy", k.y, k.out_y), ("cf", k.gf, k.out_f), ("cx", k.gx, k.out_x),
         ("cq", k.out_a.at[:, pl.ds(256, 384)], k.out_q), ("co", k.out_a.at[:, pl.ds(QKV, 384)], k.out_o)))}
    for name, copy in outs.items():
        ops[name] = copy.start
    order(types.SimpleNamespace(**ops))
    outs["cq"].start()
    outs["co"].start()

    for rank in range(4):
        here = slice(rank * part_rows, (rank + 1) * part_rows)
        k.kvsend[rank, :, 0:256] = k.out_a[here, 0:256].astype(BF)
        k.kvsend[rank, :, 256:384] = k.out_a[here, 512:640].astype(BF)
    tail = []
    for i, peer in enumerate((k.sib, k.far, cross)):
        tail.append(pltpu.make_async_remote_copy(
            k.kvsend.at[peer], k.kvgot.at[t], k.kv_s.at[3 + i], k.kv_r.at[3 + i], (f, peer), MESH))
    own = pltpu.make_async_copy(k.kvsend.at[t], k.kvgot.at[t], k.loc.at[9])
    own.start()
    for copy in tail:
        copy.start()
    for copy in tail:
        copy.wait_recv()
    own.wait()
    got = [k.kvgot[rank].astype(F32) for rank in range(4)]
    k.out_n[...] = got[0][:, 256:384] + got[1][:, 256:384] + got[2][:, 256:384] + got[3][:, 256:384]
    for base, out in ((0, k.out_k), (128, k.out_v)):
        heads = [got[0][:, base:base + 64]]
        for rank in range(3):
            heads.append(got[rank][:, base + 64:base + 128] + got[rank + 1][:, base:base + 64])
        out[:, 0:128] = jnp.concatenate(heads[0:2], axis=1)
        out[:, 128:256] = jnp.concatenate(heads[2:4], axis=1)
        out[:, 256:320] = got[3][:, base + 64:base + 128]
    for copy in tail:
        copy.wait_send()
    for name in ("x", "n2"):
        for b in range(MB):
            ex[name, b].drain()
    for chunk in scatter.values():
        chunk.drain()
    for piece in ring.values():
        piece.drain()
    for copy in outs.values():
        copy.wait()


def backward(k, ex, ring, sums, tree_sum, two_blocks, normed, pick, head_masks, chunk_of, ops, each):
    t = k.t
    lane = lax.broadcasted_iota(jnp.int32, (8, 128), 1)[0:1]
    scatter = {
        "d0": RingSum(k, 0, k.gw, 1024, 512, k.slot_f, 1024, k.gf, 1024),
        "e0": RingSum(k, 1, k.gw, 0, 1024, k.slot_f, 0, k.gf, 0),
        "d1": RingSum(k, 2, k.gw, 2304, 384, k.slot_f, 2304, k.gf, 2304),
        "e1": RingSum(k, 3, k.gw, 1536, 768, k.slot_f, 1536, k.gf, 1536),
        "o": RingSum(k, 4, k.wf, 640, 384, k.slot_a, 640, k.out_a, 640),
        "a0": RingSum(k, 5, k.wf, 0, 512, k.slot_a, 0, k.out_a, 0),
        "a1": RingSum(k, 6, k.wf, 512, 128, k.slot_a, 512, k.out_a, 512),
    }

    def gate_up(b, c):
        low, high = SPANS[c]
        width = high - low

        def body(i):
            r = pl.ds(pl.multiple_of(b * 512 + i * 256, 256), 256)
            both = dot(k.n2all[r, :], k.wf[:, WF[c][0]:WF[c][2]], 1, 0)
            gate, up = both[:, 0:width], both[:, width:2 * width]
            s = 1.0 / (1.0 + jnp.exp(-gate))
            silu = gate * s
            k.m[r, low:high] = (silu * up).astype(BF)
            k.ab[r, AB[c][0]:AB[c][1]] = (up * s * (1.0 + gate * (1.0 - s))).astype(BF)
            k.ab[r, AB[c][1]:AB[c][2]] = silu.astype(BF)

        loop(2, body)

    def grad_down(c):
        low, high = SPANS[c]

        def body(i):
            k.gw[rows(i, 256, 256), WF[c][2]:WF[c][3]] = dot(
                k.dyall[:, rows(i, 256, 256)], k.m[:, low:high], 0, 0).astype(BF)

        if c == 0:
            for b in range(MB):
                ex["dy", b].drain()
        loop(5, body)
        scatter["d" + str(c)].start()

    def hidden_grads(b, c):
        def body(i):
            r = pl.ds(pl.multiple_of(b * 512 + i * 256, 256), 256)
            product = dot(k.dyall[r, :], k.wf[:, WF[c][2]:WF[c][3]], 1, 0)
            for i in range(2):
                lanes = slice(AB[c][i], AB[c][i + 1])
                k.ab[r, lanes] = (product * k.ab[r, lanes].astype(F32)).astype(BF)

        loop(2, body)

    def second_norm_part(b):
        two_blocks(b, lambda r: sum(
            dot(k.ab[r, AB[c][0]:AB[c][2]], k.wf[:, WF[c][0]:WF[c][2]], 1, 1) for c in range(2)))
        tree_sum("dn2", 2, 0, b)

    def grad_gate_up(c):
        def body(i):
            k.gw[rows(i, 256, 256), WF[c][0]:WF[c][2]] = dot(
                k.n2all[:, rows(i, 256, 256)], k.ab[:, AB[c][0]:AB[c][2]], 0, 0).astype(BF)

        loop(5, body)
        scatter["e" + str(c)].start()

    def finish_hidden_grad(b):
        total = sums["dn2", b]
        total.wait()

        def body(i):
            r = rows(i, 32, 32)
            own = pl.ds(pl.multiple_of(b * 512 + t * 128 + i * 32, 32), 32)
            local = pl.ds(pl.multiple_of(b * 128 + i * 32, 32), 32)
            grad, hid = total.value(r), k.hid[local, :]
            scale = lax.rsqrt(jnp.mean(hid * hid, axis=-1, keepdims=True) + EPSILON)
            k.ggain[1:2, :] += jnp.sum(hid * scale * grad, axis=0, keepdims=True)
            weighted = k.gains[1:2, :] * grad
            dh = (
                k.dyall[own, :].astype(F32)
                + scale * weighted
                - hid * (scale * scale * scale) * jnp.mean(hid * weighted, axis=-1, keepdims=True)
            )
            k.gx[local, :] = dh
            k.dyall[own, :] = dh.astype(BF)

        loop(4, body)
        ex["dh", b].start()
        total.drain()

    def output_part(b):
        two_blocks(b, lambda r: sum(
            dot(k.m[r, SPANS[c][0]:SPANS[c][1]], k.wf[:, WF[c][2]:WF[c][3]], 1, 1) for c in range(2)))
        tree_sum("out", 4, 1, b)

    def finish_output(b):
        total = sums["out", b]
        total.wait()

        def body(i):
            r = rows(i, 32, 32)
            local = pl.ds(pl.multiple_of(b * 128 + i * 32, 32), 32)
            k.y[local, :] = (k.hid[local, :] + total.value(r)).astype(BF)

        loop(4, body)
        total.drain()

    def grad_out():
        for name in ("g0", "u0", "d0", "g1", "u1", "d1"):
            ring[name].drain()

        def body(i):
            k.wf[rows(i, 256, 256), 640:1024] = dot(k.dyall[:, rows(i, 256, 256)], k.att[...], 0, 0).astype(BF)

        loop(5, body)
        scatter["o"].start()

    def mixed_grad(b):
        def body(i):
            r = pl.ds(pl.multiple_of(b * 512 + i * 256, 256), 256)
            k.datt[r, :] = dot(k.dyall[r, :], k.wa[:, 640:1024], 1, 0).astype(BF)

        loop(2, body)

    def attend_back(b):
        base = b * 512
        k.dq[...] = jnp.zeros_like(k.dq)
        k.dkv[...] = jnp.zeros_like(k.dkv)

        def head(h):
            parity, group, in_half, straight = head_masks(h)
            keys, values = pick(b, h, slice(0, 128)), pick(b, h, slice(128, 256))
            for low, high, width in ((0, 128, 128), (128, 512, 512)):
                q = k.qkv[base + low:base + high, chunk_of(h, 256)]
                grad = k.datt[base + low:base + high, chunk_of(h, 0)]
                prob = k.prob[b * 5 + h, low:high, 0:width]
                grad_prob = dot(grad, values[0:width], 1, 1)
                wide = prob.astype(F32)
                delta = jnp.sum(wide * grad_prob, axis=-1, keepdims=True)
                ds = (wide * (grad_prob - delta)).astype(BF)
                k.dq[low:high, chunk_of(h, 0)] += dot(ds, keys[0:width], 1, 0)
                dk = dot(ds, q, 0, 0) * in_half
                dv = dot(prob, grad, 0, 0) * in_half
                k.dkv[0:width, 0:128] += jnp.where(group == parity, dk, pltpu.roll(dk, 64, 1))
                k.dkv[0:width, 128:256] += jnp.where(group == parity, dv, pltpu.roll(dv, 64, 1))

        loop(5, head)

        def body(i):
            r = pl.ds(pl.multiple_of(base + i * 128, 128), 128)
            local = rows(i, 128, 128)
            cos, sin = k.cs[r, 0:128], k.cs[r, 128:256]
            u = k.dkv[local, 0:128]
            k.qkv[r, 0:128] = (u * cos - swap_halves(u) * sin).astype(BF)
            k.qkv[r, 128:256] = k.dkv[local, 128:256].astype(BF)
            for chunk in range(3):
                u = k.dq[local, chunk * 128:(chunk + 1) * 128]
                u = (u * cos - swap_halves(u) * sin) * HD ** (-0.5)
                k.qkv[r, 256 + chunk * 128:384 + chunk * 128] = u.astype(BF)

        loop(4, body)

    def first_norm_part(b):
        two_blocks(b, lambda r: dot(k.qkv[r, :], k.wa[:, 0:QKV], 1, 1))
        tree_sum("dn1", 6, 0, b)

    def first_norm_again(b):
        if b == 0:
            for other in range(MB):
                ex["dh", other].drain()

        def body(i):
            r = pl.ds(pl.multiple_of(b * 512 + i * 32, 32), 32)
            k.dyall[r, :] = (normed(r) * k.gains[0:1, :]).astype(BF)

        loop(16, body)

    def first_gain(b):
        def body(i):
            unit = normed(pl.ds(pl.multiple_of(b * 512 + i * 32, 32), 32))
            spot = pl.ds(pl.multiple_of((i % 4) * 32, 32), 32)
            grad = k.part[b, (i // 4) % 2, i // 8, spot, :].astype(F32)
            k.ggain[0:1, :] += jnp.sum(unit * grad, axis=0, keepdims=True)

        loop(16, body)

    def grad_first():
        def body(i):
            k.wf[rows(i, 256, 256), 0:512] = dot(k.dyall[:, rows(i, 256, 256)], k.qkv[:, 0:512], 0, 0).astype(BF)

        loop(5, body)
        scatter["a0"].start()

    def grad_last():
        for i in range(10):
            r = slice(i * 128, (i + 1) * 128)
            turned = jnp.concatenate(
                [jnp.zeros((64, 128), F32), k.ggain[:, r], jnp.zeros((56, 128), F32)], axis=0).T
            product = dot(k.dyall[:, r], k.qkv[:, 512:640], 0, 0)
            k.wf[r, 512:640] = (product + turned).astype(BF)
        scatter["a1"].start()

    def finish_input(b):
        total = sums["dn1", b]
        total.wait()

        def body(i):
            r = rows(i, 32, 32)
            own = pl.ds(pl.multiple_of(b * 512 + t * 128 + i * 32, 32), 32)
            local = pl.ds(pl.multiple_of(b * 128 + i * 32, 32), 32)
            grad, source = total.value(r), k.xall[own, :].astype(F32)
            scale = lax.rsqrt(jnp.mean(source * source, axis=-1, keepdims=True) + EPSILON)
            weighted = k.gains[0:1, :] * grad
            k.gx[local, :] = (
                k.gx[local, :]
                + scale * weighted
                - source * (scale * scale * scale) * jnp.mean(source * weighted, axis=-1, keepdims=True)
            )

        loop(4, body)
        total.drain()

    for c in range(2):
        each("gu" + str(c), functools.partial(lambda c, b: gate_up(b, c), c))
        each("hg" + str(c), functools.partial(lambda c, b: hidden_grads(b, c), c))
        ops["gd" + str(c)] = functools.partial(grad_down, c)
        ops["gg" + str(c)] = functools.partial(grad_gate_up, c)
    each("sn", second_norm_part)
    each("dm", lambda b: sums["dn2", b].middle())
    each("fd", finish_hidden_grad)
    each("df", lambda b: ex["dh", b].forward())
    each("dd", lambda b: ex["dh", b].finish())
    each("yp", output_part)
    each("ym", lambda b: sums["out", b].middle())
    each("fy", finish_output)
    ops["go"] = grad_out
    each("mg", mixed_grad)
    each("ba", attend_back)
    each("fp", first_norm_part)
    each("na", first_norm_again)
    each("fg", first_gain)
    ops["gf"], ops["gl"] = grad_first, grad_last
    each("im", lambda b: sums["dn1", b].middle())
    each("fi", finish_input)
    for name, chunk in scatter.items():
        ops["r" + name] = chunk.pump
    return scatter


def layer(n, shard, arrays):
    def shape(dims, kind=BF):
        return jax.ShapeDtypeStruct(dims, kind)

    inputs = ("xin", "dyin", "wq", "wo", "wk", "wv", "gn", "gate", "up", "down", "seg", "pos", "par", "freq")
    spaces = dict(xin=pl.ANY, dyin=pl.ANY, gate=pl.ANY, up=pl.ANY, down=pl.ANY, par=pltpu.SMEM)
    outputs = {
        "out_y": shape((256, 1280)),
        "out_x": shape((256, 1280), F32),
        "out_f": shape((shard, 2688), F32),
        "out_q": shape((shard, 384), F32),
        "out_o": shape((shard, 384), F32),
        "out_k": shape((shard // 4, 320), F32),
        "out_v": shape((shard // 4, 320), F32),
        "out_n": shape((shard // 4, 128), F32),
    }
    far_outputs = ("out_y", "out_x", "out_f", "out_q", "out_o")
    half = shard // 2
    dma = pltpu.SemaphoreType.DMA
    scratch = {
        "wa": pltpu.VMEM((1280, AW), BF),
        "wf": pltpu.VMEM((1280, 2688), BF),
        "xall": pltpu.VMEM((1024, 1280), BF),
        "dyall": pltpu.VMEM((1024, 1280), BF),
        "n2all": pltpu.VMEM((1024, 1280), BF),
        "kvr": pltpu.VMEM((4, shard // 4, 384), BF),
        "qkv": pltpu.VMEM((1024, QKV), BF),
        "kvrot": pltpu.VMEM((1024, 256), BF),
        "att": pltpu.VMEM((1024, 384), BF),
        "datt": pltpu.VMEM((1024, 384), BF),
        "prob": pltpu.VMEM((10, 512, 512), BF),
        "bias": pltpu.VMEM((1024, 512), BF),
        "cs": pltpu.VMEM((1024, 256), F32),
        "gains": pltpu.VMEM((8, 1280), F32),
        "ggain": pltpu.VMEM((8, 1280), F32),
        "m": pltpu.VMEM((1024, 896), BF),
        "ab": pltpu.VMEM((1024, 1792), BF),
        "part": pltpu.VMEM((2, 2, 2, 128, 1280), BF),
        "near": pltpu.VMEM((2, 2, 2, 128, 1280), BF),
        "half": pltpu.VMEM((2, 2, 128, 1280), BF),
        "far_in": pltpu.VMEM((2, 2, 128, 1280), BF),
        "hid": pltpu.VMEM((256, 1280), F32),
        "gw": pltpu.VMEM((1280, 2688), BF),
        "slot_f": pltpu.VMEM((2, n - 1, half, 2688), BF),
        "slot_a": pltpu.VMEM((2, n - 1, half, AW), BF),
        "dq": pltpu.VMEM((512, 384), F32),
        "dkv": pltpu.VMEM((512, 256), F32),
        "y": pltpu.VMEM((256, 1280), BF),
        "gx": pltpu.VMEM((256, 1280), F32),
        "gf": pltpu.VMEM((shard, 2688), F32),
        "out_a": pltpu.VMEM((shard, AW), F32),
        "kvgot": pltpu.VMEM((4, shard // 4, 384), BF),
        "kvsend": pltpu.VMEM((4, shard // 4, 384), BF),
        "loc": dma((16,)),
        "kv_s": dma((6,)), "kv_r": dma((6,)),
        "ex_s": dma((8, 3)), "ex_r": dma((8, 3)),
        "ts_s": dma((8, 2)), "ts_r": dma((8, 2)),
        "ga_s": dma((16, n // 2)), "ga_r": dma((16, n // 2)),
        "rs_s": dma((14, n - 1)), "rs_r": dma((14, n - 1)),
    }
    names = inputs + tuple(outputs) + tuple(scratch)
    return pl.pallas_call(
        functools.partial(layer_kernel, n, shard, names),
        out_shape=tuple(outputs.values()),
        in_specs=[pl.BlockSpec(memory_space=spaces.get(name, pltpu.VMEM)) for name in inputs],
        out_specs=tuple(pl.BlockSpec(memory_space=pl.ANY if name in far_outputs else pltpu.VMEM) for name in outputs),
        scratch_shapes=list(scratch.values()),
        compiler_params=pltpu.CompilerParams(
            collective_id=0, has_side_effects=True, vmem_limit_bytes=67043328),
        name="layer",
    )(*arrays)


def fused_device(mesh_n, inputs, cotangent, segment_ids, parents, positions, norm1_gain, w_query, w_key,
                 w_value, w_out, norm2_gain, w_gate, w_up, w_down):
    shard = w_query.shape[0]
    steps = 1.0 / np.float32(ROPE_BASE) ** (np.arange(32, dtype=np.float32) / 32)
    freq = np.broadcast_to(np.tile(steps, 4)[None], (8, 128)).astype(np.float32)
    gains = jnp.stack([norm1_gain, norm2_gain]).astype(F32)
    outs = layer(mesh_n, shard, (
        inputs, cotangent, w_query, w_out.T, w_key, w_value, gains, w_gate, w_up, w_down.T, segment_ids, positions,
        parents, freq))
    y, gx, gf, gq, go, key, value, gains = outs
    gg, gu, gd = (
        jnp.concatenate([gf[:, WF[c][i]:WF[c][i + 1]] for c in range(2)], axis=1) for i in range(3))
    return (
        y.reshape(2, 128, 1280), gx.reshape(2, 128, 1280), gains[:, 64], gq[:, 0:320], key, value, go[:, 0:320].T, gains[:, 65], gg, gu, gd.T)


def across_rows(left_side, right_side):
    return lax.dot_general(
        left_side, right_side, (((0,), (0,)), ((), ())), preferred_element_type=jnp.float32
    )


def against_rows(left_side, right_side):
    return lax.dot_general(
        left_side, right_side, (((1,), (1,)), ((), ())), preferred_element_type=jnp.float32
    )


def norm_scale(values):
    return lax.rsqrt(jnp.mean(values * values, axis=-1, keepdims=True) + EPSILON)


def rotate(values, places, turning):
    half_width = HD // 2
    frequency = 1.0 / ROPE_BASE ** (jnp.arange(half_width, dtype=jnp.float32) / half_width)
    angles = places.astype(jnp.float32)[..., None] * frequency
    cosine = jnp.cos(angles)[..., None, :]
    sine_part = turning * jnp.sin(angles)[..., None, :]
    shaped = values.reshape(values.shape[:-1] + (values.shape[-1] // HD, HD))
    first_half = shaped[..., :half_width]
    second_half = shaped[..., half_width:]
    turned = jnp.concatenate(
        [
            first_half * cosine - second_half * sine_part,
            second_half * cosine + first_half * sine_part,
        ],
        axis=-1,
    )
    return turned.reshape(values.shape)


def lineage(segment, table):
    labels = jnp.arange(13, dtype=jnp.int32)
    first_label = jnp.min(segment) // 13 * 13
    picked = (segment - first_label)[:, None] == labels[None, :]
    parent = jnp.sum(jnp.where(picked, table[None, :], 0), axis=1)
    picked_two = (parent - first_label)[:, None] == labels[None, :]
    grand_parent = jnp.sum(jnp.where(picked_two, table[None, :], 0), axis=1)
    return (parent, grand_parent)


def allowed_pairs(block_segment, block_parent, block_grand, block_places, segment, places):
    same_path = (
        (segment[None, :] == block_segment[:, None])
        | (segment[None, :] == block_parent[:, None])
        | (segment[None, :] == block_grand[:, None])
    )
    return same_path & (places[None, :] <= block_places[:, None])


def rows_in(values):
    return lax.all_gather(values, "tp", axis=0, tiled=True)


def rows_out(term):
    return lax.psum_scatter(
        term.astype(jnp.bfloat16), "tp", scatter_dimension=0, tiled=True
    ).astype(jnp.float32)


def fetch_weights(w_query, w_out, w_key, w_value, norm1_gain, norm2_gain, w_gate, w_up, w_down):
    query_full, out_full = (
        lax.all_gather(w_query, "fsdp", axis=0, tiled=True),
        lax.all_gather(w_out, "fsdp", axis=1, tiled=True),
    )
    key_full, value_full, gain_one, gain_two = (
        lax.all_gather(w_key, ("fsdp", "tp"), axis=0, tiled=True),
        lax.all_gather(w_value, ("fsdp", "tp"), axis=0, tiled=True),
        lax.all_gather(norm1_gain, ("fsdp", "tp"), axis=0, tiled=True),
        lax.all_gather(norm2_gain, ("fsdp", "tp"), axis=0, tiled=True),
    )
    gate_full, up_full, down_full = (
        lax.all_gather(w_gate, "fsdp", axis=0, tiled=True),
        lax.all_gather(w_up, "fsdp", axis=0, tiled=True),
        lax.all_gather(w_down, "fsdp", axis=1, tiled=True),
    )
    return (
        query_full,
        key_full,
        value_full,
        out_full,
        gain_one.astype(jnp.float32),
        gain_two.astype(jnp.float32),
        gate_full,
        up_full,
        down_full,
    )


def reduce_grads(gradients):
    grad_q, grad_k, grad_v, grad_o, grad_g1, grad_g2, grad_gt, grad_u, grad_dn = gradients
    part_q, part_o, part_gt, part_u, part_dn = (
        lax.psum_scatter(grad_q, "fsdp", scatter_dimension=0, tiled=True),
        lax.psum_scatter(grad_o, "fsdp", scatter_dimension=1, tiled=True),
        lax.psum_scatter(grad_gt, "fsdp", scatter_dimension=0, tiled=True),
        lax.psum_scatter(grad_u, "fsdp", scatter_dimension=0, tiled=True),
        lax.psum_scatter(grad_dn, "fsdp", scatter_dimension=1, tiled=True),
    )
    part_k, part_v, part_g1, part_g2 = (
        lax.psum_scatter(grad_k, ("fsdp", "tp"), scatter_dimension=0, tiled=True),
        lax.psum_scatter(grad_v, ("fsdp", "tp"), scatter_dimension=0, tiled=True),
        lax.psum_scatter(grad_g1, ("fsdp", "tp"), scatter_dimension=0, tiled=True),
        lax.psum_scatter(grad_g2, ("fsdp", "tp"), scatter_dimension=0, tiled=True),
    )
    return (part_q, part_k, part_v, part_o, part_g1, part_g2, part_gt, part_u, part_dn)


def attention_forward(query_heads, keys_heads, values_heads, segment, parent, grand_parent, places):
    group_rows, local_heads = (query_heads.shape[0], query_heads.shape[1])
    block_rows = min(512, group_rows)
    block_count = group_rows // block_rows
    scale = HD ** (-0.5)

    def one_block(pieces):
        query_block, block_segment, block_parent, block_grand, block_places = pieces
        allowed = allowed_pairs(
            block_segment, block_parent, block_grand, block_places, segment, places
        )
        scores = (
            jnp.einsum("qhd,khd->hqk", query_block, keys_heads, preferred_element_type=jnp.float32)
            * scale
        )
        scores = jnp.where(allowed[None], scores, MASKED)
        row_peak = jnp.max(scores, axis=-1, keepdims=True)
        weights_row = jnp.exp(scores - row_peak)
        row_total = jnp.sum(weights_row, axis=-1, keepdims=True)
        probability = weights_row / row_total
        mixed = jnp.einsum(
            "hqk,khd->qhd",
            probability.astype(jnp.bfloat16),
            values_heads,
            preferred_element_type=jnp.float32,
        )
        return (mixed.astype(jnp.bfloat16), (row_peak + jnp.log(row_total))[..., 0])

    pieces = (
        query_heads.reshape(block_count, block_rows, local_heads, HD),
        segment.reshape(block_count, block_rows),
        parent.reshape(block_count, block_rows),
        grand_parent.reshape(block_count, block_rows),
        places.reshape(block_count, block_rows),
    )
    mixed, log_total = lax.map(one_block, pieces)
    return (mixed.reshape(group_rows, local_heads * HD), log_total)


def attention_backward(
    query_heads,
    keys_heads,
    values_heads,
    grad_mixed,
    log_total,
    segment,
    parent,
    grand_parent,
    places,
):
    group_rows, local_heads = (query_heads.shape[0], query_heads.shape[1])
    block_rows = min(512, group_rows)
    block_count = group_rows // block_rows
    scale = HD ** (-0.5)

    def one_block(running, pieces):
        key_grad, value_grad = running
        (
            query_block,
            out_block,
            block_log,
            block_segment,
            block_parent,
            block_grand,
            block_places,
        ) = pieces
        allowed = allowed_pairs(
            block_segment, block_parent, block_grand, block_places, segment, places
        )
        scores = (
            jnp.einsum("qhd,khd->hqk", query_block, keys_heads, preferred_element_type=jnp.float32)
            * scale
        )
        probability = jnp.where(allowed[None], jnp.exp(scores - block_log[..., None]), 0.0)
        grad_prob = jnp.einsum(
            "qhd,khd->hqk", out_block, values_heads, preferred_element_type=jnp.float32
        )
        row_delta = jnp.sum(probability * grad_prob, axis=-1, keepdims=True)
        grad_score = (scale * probability * (grad_prob - row_delta)).astype(jnp.bfloat16)
        query_grad = jnp.einsum(
            "hqk,khd->qhd", grad_score, keys_heads, preferred_element_type=jnp.float32
        )
        key_grad = key_grad + jnp.einsum(
            "hqk,qhd->khd", grad_score, query_block, preferred_element_type=jnp.float32
        )
        value_grad = value_grad + jnp.einsum(
            "hqk,qhd->khd",
            probability.astype(jnp.bfloat16),
            out_block,
            preferred_element_type=jnp.float32,
        )
        return ((key_grad, value_grad), query_grad)

    zeros_heads = jnp.zeros((group_rows, local_heads, HD), jnp.float32)
    pieces = (
        query_heads.reshape(block_count, block_rows, local_heads, HD),
        grad_mixed.reshape(block_count, block_rows, local_heads, HD),
        log_total,
        segment.reshape(block_count, block_rows),
        parent.reshape(block_count, block_rows),
        grand_parent.reshape(block_count, block_rows),
        places.reshape(block_count, block_rows),
    )
    (key_grad, value_grad), query_grad = lax.scan(one_block, (zeros_heads, zeros_heads), pieces)
    return (query_grad.reshape(group_rows, local_heads, HD), key_grad, value_grad)


def per_device(
    inputs,
    cotangent,
    segment_ids,
    parents,
    positions,
    norm1_gain,
    w_query,
    w_key,
    w_value,
    w_out,
    norm2_gain,
    w_gate,
    w_up,
    w_down,
):
    head_rank = lax.axis_index("tp")
    local_heads = w_query.shape[1] // HD
    key_head = (head_rank * local_heads + jnp.arange(local_heads, dtype=jnp.int32)) // (H // KV)
    head_choice = (key_head[:, None] == jnp.arange(KV, dtype=jnp.int32)[None, :]).astype(
        jnp.float32
    )
    choice_low = head_choice.astype(jnp.bfloat16)
    outputs = []
    input_grads = []
    shards = None
    for batch_index in range(MB):
        weights = fetch_weights(
            w_query, w_out, w_key, w_value, norm1_gain, norm2_gain, w_gate, w_up, w_down
        )
        (
            query_full,
            key_full,
            value_full,
            out_full,
            gain_one,
            gain_two,
            gate_full,
            up_full,
            down_full,
        ) = weights
        source = inputs[batch_index].astype(jnp.float32)
        segment = segment_ids[batch_index]
        places = positions[batch_index]
        parent, grand_parent = lineage(segment, parents[batch_index])
        norm_one = norm_scale(source)
        normed = (source * norm_one * gain_one).astype(jnp.bfloat16)
        normed_all = rows_in(normed)
        queries = rotate(
            jnp.dot(normed_all, query_full, preferred_element_type=jnp.float32), places, 1.0
        ).astype(jnp.bfloat16)
        keys_all = rotate(
            jnp.dot(normed_all, key_full, preferred_element_type=jnp.float32), places, 1.0
        ).astype(jnp.bfloat16)
        values_all = jnp.dot(normed_all, value_full, preferred_element_type=jnp.float32).astype(
            jnp.bfloat16
        )
        group_rows = keys_all.shape[0]
        keys_heads = jnp.einsum(
            "gkd,hk->ghd",
            keys_all.reshape(group_rows, KV, HD),
            choice_low,
            preferred_element_type=jnp.float32,
        ).astype(jnp.bfloat16)
        values_heads = jnp.einsum(
            "gkd,hk->ghd",
            values_all.reshape(group_rows, KV, HD),
            choice_low,
            preferred_element_type=jnp.float32,
        ).astype(jnp.bfloat16)
        query_heads = queries.reshape(group_rows, local_heads, HD)
        attended, log_total = attention_forward(
            query_heads, keys_heads, values_heads, segment, parent, grand_parent, places
        )
        hidden = source + rows_out(jnp.dot(attended, out_full, preferred_element_type=jnp.float32))
        norm_two = norm_scale(hidden)
        normed_two = (hidden * norm_two * gain_two).astype(jnp.bfloat16)
        normed_two_all = rows_in(normed_two)
        gate_pre = jnp.dot(normed_two_all, gate_full, preferred_element_type=jnp.float32)
        upward = jnp.dot(normed_two_all, up_full, preferred_element_type=jnp.float32)
        sigmoid_gate = jax.nn.sigmoid(gate_pre)
        activated = gate_pre * sigmoid_gate
        product = (activated * upward).astype(jnp.bfloat16)
        output = hidden + rows_out(jnp.dot(product, down_full, preferred_element_type=jnp.float32))
        grad_hidden = cotangent[batch_index].astype(jnp.float32)
        grad_branch = rows_in(grad_hidden.astype(jnp.bfloat16))
        grad_product = against_rows(grad_branch, down_full)
        grad_down_w = across_rows(product, grad_branch)
        grad_gate_pre = (
            grad_product * upward * sigmoid_gate * (1.0 + gate_pre * (1.0 - sigmoid_gate))
        ).astype(jnp.bfloat16)
        grad_upward = (grad_product * activated).astype(jnp.bfloat16)
        grad_gate_w = across_rows(normed_two_all, grad_gate_pre)
        grad_up_w = across_rows(normed_two_all, grad_upward)
        grad_normed_two = rows_out(
            against_rows(grad_gate_pre, gate_full) + against_rows(grad_upward, up_full)
        )
        gain_two_grad = jnp.sum(hidden * norm_two * grad_normed_two, axis=0)
        weighted_two = gain_two * grad_normed_two
        grad_hidden = (
            grad_hidden
            + norm_two * weighted_two
            - hidden
            * (norm_two * norm_two * norm_two)
            * jnp.mean(hidden * weighted_two, axis=-1, keepdims=True)
        )
        grad_attn = rows_in(grad_hidden.astype(jnp.bfloat16))
        grad_out_w = across_rows(attended, grad_attn)
        grad_mixed = (
            against_rows(grad_attn, out_full)
            .astype(jnp.bfloat16)
            .reshape(group_rows, local_heads, HD)
        )
        query_grad, key_grad, value_grad = attention_backward(
            query_heads,
            keys_heads,
            values_heads,
            grad_mixed,
            log_total,
            segment,
            parent,
            grand_parent,
            places,
        )
        key_part = jnp.einsum(
            "ghd,hk->gkd", key_grad, head_choice, precision=lax.Precision.HIGHEST
        ).reshape(group_rows, KV * HD)
        value_part = jnp.einsum(
            "ghd,hk->gkd", value_grad, head_choice, precision=lax.Precision.HIGHEST
        ).reshape(group_rows, KV * HD)
        key_part = rotate(key_part, places, -1.0)
        query_raw = rotate(query_grad.reshape(group_rows, local_heads * HD), places, -1.0).astype(
            jnp.bfloat16
        )
        grad_query_w = across_rows(normed_all, query_raw)
        normed_term = against_rows(query_raw, query_full)
        grad_normed = lax.psum_scatter(
            normed_term.astype(jnp.bfloat16), "tp", scatter_dimension=0, tiled=True
        ).astype(jnp.float32)
        key_sum = lax.psum_scatter(
            key_part.astype(jnp.bfloat16), "tp", scatter_dimension=0, tiled=True
        )
        value_sum = lax.psum_scatter(
            value_part.astype(jnp.bfloat16), "tp", scatter_dimension=0, tiled=True
        )
        grad_key_w = across_rows(normed, key_sum)
        grad_value_w = across_rows(normed, value_sum)
        grad_normed = (
            grad_normed + against_rows(key_sum, key_full) + against_rows(value_sum, value_full)
        )
        gain_one_grad = jnp.sum(source * norm_one * grad_normed, axis=0)
        weighted_one = gain_one * grad_normed
        grad_source = (
            grad_hidden
            + norm_one * weighted_one
            - source
            * (norm_one * norm_one * norm_one)
            * jnp.mean(source * weighted_one, axis=-1, keepdims=True)
        )
        gradients = (
            grad_query_w,
            grad_key_w,
            grad_value_w,
            grad_out_w,
            gain_one_grad,
            gain_two_grad,
            grad_gate_w,
            grad_up_w,
            grad_down_w,
        )
        output, grad_source, gradients = (output.astype(jnp.bfloat16), grad_source, gradients)
        outputs.append(output)
        input_grads.append(grad_source)
        summed = reduce_grads(gradients)
        shards = summed if batch_index == 0 else jax.tree.map(jnp.add, shards, summed)
    return (
        jnp.stack(outputs),
        jnp.stack(input_grads),
        shards[4],
        shards[0],
        shards[1],
        shards[2],
        shards[3],
        shards[5],
        shards[6],
        shards[7],
        shards[8],
    )


def solution(mesh):
    placed = (
        P(None, ("fsdp", "tp"), None),
        P(None, ("fsdp", "tp"), None),
        P(None, "fsdp"),
        P(None, "fsdp"),
        P(None, "fsdp"),
        P(("fsdp", "tp")),
        P("fsdp", "tp"),
        P(("fsdp", "tp"), None),
        P(("fsdp", "tp"), None),
        P("tp", "fsdp"),
        P(("fsdp", "tp")),
        P("fsdp", "tp"),
        P("fsdp", "tp"),
        P("tp", "fsdp"),
    )
    ring = mesh.shape["fsdp"]
    body = functools.partial(fused_device, ring) if ring == 8 else per_device
    return jax.shard_map(
        body,
        mesh=mesh,
        in_specs=placed,
        out_specs=(
            P(None, ("fsdp", "tp"), None),
            P(None, ("fsdp", "tp"), None),
            P(("fsdp", "tp")),
            P("fsdp", "tp"),
            P(("fsdp", "tp"), None),
            P(("fsdp", "tp"), None),
            P("tp", "fsdp"),
            P(("fsdp", "tp")),
            P("fsdp", "tp"),
            P("fsdp", "tp"),
            P("tp", "fsdp"),
        ),
        check_vma=False,
    )
```
